32 devices in a mesh: tm: 4 (over y, x), space: 8 (over z, core).
Axes of the slice: x: 2, y: 2, z: 4, core: 2. Of those that a mesh axis runs over, the one named last changes fastest.
Arguments:
- initial_state: float32 [16, 256, 256], P('space'), may hold values from -6 to 6
- capacity: float32 [16, 256, 256], P('space'), may hold values from 0.5 to 2
- source: float32 [16, 256, 256], P('space'), may hold values from -6 to 6
- control: float32 [4, 16], P('tm'), may hold values from -2 to 2
- segment_index: int32 [16, 256], P('space'), may hold values from 0 to 15
Outputs:
- slice_ends: float32 [4, 16, 256, 256], P('tm', 'space')
The draws below stay inside these ranges and needn't reach their ends.
All inputs are finite; a program needn't handle non-finite values.
Results may differ from the reference program's by a relative error of at most 0.0001.
Values sent between devices are 32-bit elements; how exact they have to be, the bound alone decides.
A program may use at most 64 MiB of HBM per device.

```python
import math
import jax
import jax.numpy as jnp

NY = 256
NZ = 256
FINE = 1
SWEEPS = 6
CORRECTIONS = 2
SEGMENTS = 16
SLICES = 4
NX = 16


def touch_ends(result, key, smallest, high):
    longest = result.shape.index(max(result.shape))
    spots = []
    for shift in (0, 1):
        where = [jax.random.randint(jax.random.fold_in(key, axis), (), 0, length) for axis, length in enumerate(result.shape)]
        where[longest] = (where[longest] + shift) % result.shape[longest]
        spots.append(tuple(where))
    return result.at[spots[0]].set(smallest).at[spots[1]].set(high)


def block_levels(rng, dims, shards, least, top_value):
    gain, own = 1.0, jax.random.fold_in(rng, 6)
    for dim, blocks in shards:
        steps = jnp.exp(jax.random.uniform(jax.random.fold_in(own, dim), (blocks,), jnp.float32, least / len(shards), top_value / len(shards)))
        gain = gain * jnp.repeat(steps, dims[dim] // blocks).reshape([-1 if axis == dim else 1 for axis in range(len(dims))])
    return gain


def centred(stream_key, extent, spread, most, cuts=(), kind=jnp.bfloat16):
    result = spread * jax.random.normal(stream_key, extent, jnp.float32)
    if cuts:
        result = result * block_levels(stream_key, extent, cuts, -0.22, 0.18)
    return jnp.clip(result, -most, most).astype(kind)


def setup_inputs(seed: int = 0) -> dict:
    keys = jax.random.split(jax.random.key(seed), 6)
    return {
        "initial_state": centred(keys[0], (NX, NY, NZ), 1.0, 6.0, ((0, 8),), jnp.float32),
        "capacity": jnp.clip(jnp.exp(math.log(2.0) - 1.3862944 * jax.random.uniform(keys[1], (NX, NY, NZ), jnp.float32) ** block_levels(keys[1], (NX, NY, NZ), ((0, 8),), -0.2, 0.2)), 0.5, 2.0),
        "source": centred(keys[2], (NX, NY, NZ), 1.0, 6.0, ((0, 8),), jnp.float32),
        "control": jnp.clip(jax.random.uniform(keys[3], (SLICES, SEGMENTS), jnp.float32, -2.0, 2.0) * block_levels(keys[3], (SLICES, SEGMENTS), ((0, 4),), -0.4, 0.0), -2.0, 2.0),
        "segment_index": touch_ends(jax.random.randint(keys[4], (NX, NZ), 0, SEGMENTS), jax.random.fold_in(keys[4], 1), 0, SEGMENTS - 1).astype(jnp.int32),
    }


step_fine = 1.0
step_coarse = 0.08


def neighbours(extended):
    core = extended[1:-1]
    total = extended[2:] + extended[:-2]
    wide = jnp.pad(core, ((0, 0), (1, 1), (0, 0)))
    total = total + wide[:, 2:] + wide[:, :-2]
    deeper = jnp.pad(core, ((0, 0), (0, 0), (1, 1)))
    return total + deeper[:, :, 2:] + deeper[:, :, :-2]


def jacobi_sweep(extended, previous, capacity, forcing, divisor):
    return (capacity * previous + step_fine * forcing + step_fine * neighbours(extended)) / divisor


def coarse_step(extended, scale, forcing):
    core = extended[1:-1]
    return core + scale * (neighbours(extended) - 6.0 * core + forcing)


def pad_planes(field):
    return jnp.pad(field, ((1, 1), (0, 0), (0, 0)))


def boundary_forcing(source, segment_index, control_row):
    matches = segment_index[:, None, :] == jnp.arange(SEGMENTS, dtype=jnp.int32)[None, :, None]
    values = jnp.sum(jnp.where(matches, control_row[None, :, None], jnp.zeros((), source.dtype)), axis=1)
    return source + jnp.pad(values[:, None, :], ((0, 0), (0, source.shape[1] - 1), (0, 0)))


def reference(initial_state, capacity, source, control, segment_index):
    divisor = capacity + 6.0 * step_fine
    scale = step_coarse / capacity
    forcings = [boundary_forcing(source, segment_index, control[slice_index]) for slice_index in range(SLICES)]

    def fine_solve(state, forcing):
        for fine_index in range(FINE):
            iterate = state
            for sweep_index in range(SWEEPS):
                iterate = jacobi_sweep(pad_planes(iterate), state, capacity, forcing, divisor)
            state = iterate
        return state

    starts = [initial_state]
    coarse_values = []
    for slice_index in range(SLICES):
        value = coarse_step(pad_planes(starts[slice_index]), scale, forcings[slice_index])
        coarse_values.append(value)
        if slice_index + 1 < SLICES:
            starts.append(value)
    ends = []
    for correction_index in range(CORRECTIONS):
        deltas = [fine_solve(starts[n], forcings[n]) - coarse_values[n] for n in range(SLICES)]
        new_starts = [initial_state]
        new_values = []
        ends = []
        for slice_index in range(SLICES):
            value = coarse_step(pad_planes(new_starts[slice_index]), scale, forcings[slice_index])
            new_values.append(value)
            end_state = value + deltas[slice_index]
            ends.append(end_state)
            if slice_index + 1 < SLICES:
                new_starts.append(end_state)
        starts = new_starts
        coarse_values = new_values
    return jnp.stack(ends)
```

```python
import functools

import jax
import jax.numpy as jnp
from jax import lax
from jax.experimental import pallas as pl
from jax.experimental.pallas import tpu as pltpu
from jax.sharding import PartitionSpec as P

SWEEPS = 6
CORRECTIONS = 2
step_fine = 1.0
step_coarse = 0.08


def make_plan(slices):
    last = CORRECTIONS
    solves = [
        (k, n)
        for k in range(last)
        for n in range(k, slices)
        if k == last - 1 or n + 1 < slices or n == k
    ]
    slots, sent = {}, set()
    for k, n in solves:
        for j in range(SWEEPS):
            slots[(k, n, j)] = len(slots)
            sent.add((k, n, j))

    def state(k, n):
        k = min(k, n)
        key = (k, n, 0)
        if key not in slots:
            slots[key] = len(slots)
        return key

    ends = [state(last, n + 1) for n in range(slices)]
    rounds = {}
    top_coarse = max(n for k, n in solves if k == 0)
    for n in range(top_coarse):
        rounds.setdefault(n + 1, []).append(("coarse", n, state(0, n), state(0, n + 1)))
    for k, n in sorted(solves, key=lambda item: (-item[0], item[1])):
        begin = SWEEPS * k + n - k
        for j in range(1, SWEEPS + 1):
            target = (k, n, j) if j < SWEEPS else state(k + 1, n + 1)
            pair = None
            if j == SWEEPS and k < n:
                pair = (state(k + 1, n), state(k, n))
                sent.add(pair[0])
                sent.add(pair[1])
            rounds.setdefault(begin + j, []).append(("sweep", n, (k, n, j - 1), target, j, pair))
    return slots, sent, [rounds[r] for r in sorted(rounds)], ends


def kernel(plan, size, state_hbm, cap_hbm, src_hbm, ctrl_ref, seg_ref, out_hbm,
           field, forcing, base, inv, scale, source, ctrl_all,
           send_sem, recv_sem, in_sem, ctrl_send, ctrl_recv, out_send, out_recv, own_sem):
    slots, sent, rounds, ends = plan
    planes, window, own_rows, reach, rows, cols, slices, count = size
    t = lax.axis_index("tm")
    s = lax.axis_index("space")
    low_there, high_there = s > 0, s < count - 1
    first_row = pl.multiple_of(jnp.clip(t * own_rows - reach, 0, rows - window), 8)
    own_at = pl.multiple_of(t * own_rows - first_row, 8)
    inner = pl.ds(1, planes)
    first = slots[(0, 0, 0)]

    loads = []
    for index, (ref, target) in enumerate(
        ((state_hbm, field.at[first, inner]), (cap_hbm, inv), (src_hbm, source))
    ):
        loads.append(pltpu.make_async_copy(ref.at[:, pl.ds(first_row, window), :], target, in_sem.at[index]))
        loads[-1].start()

    @pl.when(jnp.logical_not(low_there))
    def _():
        for key in sorted(sent):
            field[slots[key], 0] = jnp.zeros((window, cols), jnp.float32)

    @pl.when(jnp.logical_not(high_there))
    def _():
        for key in sorted(sent):
            field[slots[key], planes + 1] = jnp.zeros((window, cols), jnp.float32)

    barrier = pltpu.get_barrier_semaphore()

    @pl.when(low_there)
    def _():
        pl.semaphore_signal(barrier, inc=1, device_id={"space": s - 1})

    @pl.when(high_there)
    def _():
        pl.semaphore_signal(barrier, inc=1, device_id={"space": s + 1})

    for hop in range(1, slices):
        pl.semaphore_signal(barrier, inc=1, device_id={"tm": lax.rem(t + hop, slices)})
    pl.semaphore_wait(barrier, slices - 1 + jnp.minimum(s, 1) + jnp.minimum(count - 1 - s, 1))

    def halo(key, side):
        slot = slots[key]
        if side == 0:
            source_plane, target_plane, other = 1, planes + 1, s - 1
        else:
            source_plane, target_plane, other = planes, 0, s + 1
        k, n, j = key
        left = CORRECTIONS * (SWEEPS - 1) + slices - (k * (SWEEPS - 1) + n + j)
        near = min(-(-left // 8) * 8, reach)
        height = min(window, own_rows + 2 * near)
        at = jnp.clip(t * own_rows - near, 0, rows - height) - first_row
        needed = pl.ds(pl.multiple_of(at, 8), height)
        return pltpu.make_async_remote_copy(
            src_ref=field.at[slot, source_plane, needed],
            dst_ref=field.at[slot, target_plane, needed],
            send_sem=send_sem.at[slot, side],
            recv_sem=recv_sem.at[slot, side],
            device_id={"space": other},
        )

    odd = lax.rem(s, 2)

    def send(key, parts=(0, 1)):
        if key in sent:
            for part in parts:
                for side, there in ((0, low_there), (1, high_there)):

                    @pl.when(jnp.logical_and(there, odd == (side + part) % 2))
                    def _():
                        halo(key, side).start()

    arrived = set()

    def arrive(key):
        if key in arrived:
            return
        arrived.add(key)
        for side, there in ((0, high_there), (1, low_there)):

            @pl.when(there)
            def _():
                halo(key, side).wait_recv()

    loads[0].wait()
    send((0, 0, 0))

    ctrl_copies = []
    for hop in range(1, slices):
        ctrl_copies.append(pltpu.make_async_remote_copy(
            src_ref=ctrl_ref,
            dst_ref=ctrl_all.at[hop],
            send_sem=ctrl_send.at[hop],
            recv_sem=ctrl_recv.at[hop],
            device_id={"tm": lax.rem(t + hop, slices)},
        ))
        ctrl_copies[-1].start()
    own_ctrl = pltpu.make_async_copy(ctrl_ref, ctrl_all.at[0], own_sem.at[0])
    own_ctrl.start()

    loads[1].wait()
    capacity = inv[...]
    scale[...] = step_coarse / capacity
    reciprocal = 1.0 / (capacity + 6.0 * step_fine)
    inv[...] = reciprocal
    loads[2].wait()
    own_ctrl.wait()
    for copy in ctrl_copies:
        copy.wait_recv()

    segment = seg_ref[...]
    segments = ctrl_ref.shape[1]
    row_id = lax.broadcasted_iota(jnp.int32, (planes, window, cols), 1) + first_row
    for n in range(slices):
        row = jnp.zeros((1, segments), jnp.float32)
        for hop in range(slices):
            row = jnp.where(lax.rem(t - n + slices, slices) == hop, ctrl_all[hop], row)
        values = jnp.zeros((planes, cols), jnp.float32)
        for k in range(segments):
            values = jnp.where(segment == k, row[:, k:k + 1], values)
        forcing[n] = source[...] + jnp.where(row_id == 0, values[:, None, :], 0.0)

    step = window // 2 if window % 16 == 0 else window
    lane = lax.broadcasted_iota(jnp.int32, (step, cols), 1)
    line = lax.broadcasted_iota(jnp.int32, (step, cols), 0)
    pieces = []
    for i in range(planes):
        p = jnp.where(odd == 1, planes - 1 - i, i)
        pieces += [(i, p, r) for r in range(0, window, step)]

    def neighbours(read, p, r):
        core = read(p + 1, r)
        if r > 0:
            above = read(p + 1, r - 1)
        else:
            above = jnp.where(line == 0, 0.0, pltpu.roll(core, 1, 0))
        if r + step < window:
            below = read(p + 1, r + 1)
        else:
            below = jnp.where(line == step - 1, 0.0, pltpu.roll(core, step - 1, 0))
        left = jnp.where(lane == 0, 0.0, pltpu.roll(core, 1, 1))
        right = jnp.where(lane == cols - 1, 0.0, pltpu.roll(core, cols - 1, 1))
        return core, read(p, r) + read(p + 2, r) + above + below + left + right

    def reader(key):
        return lambda p, r: field[slots[key], p, pl.ds(r, step)]

    def difference(new, old):
        return lambda p, r: field[slots[new], p, pl.ds(r, step)] - field[slots[old], p, pl.ds(r, step)]

    def piece(ref, p, r):
        return ref[p, pl.ds(r, step)]

    def result(n, end):
        def remote(target, source_slice):
            return pltpu.make_async_remote_copy(
                src_ref=field.at[slots[end], inner, pl.ds(own_at, own_rows)],
                dst_ref=out_hbm.at[0, :, pl.ds(pl.multiple_of(source_slice * own_rows, 8), own_rows)],
                send_sem=out_send.at[target],
                recv_sem=out_recv.at[source_slice],
                device_id={"tm": target},
            )
        return remote

    def own_copy(n):
        return pltpu.make_async_copy(
            field.at[slots[ends[n]], inner, pl.ds(own_at, own_rows)],
            out_hbm.at[0, :, pl.ds(n * own_rows, own_rows)],
            own_sem.at[1],
        )

    def emit(key):
        for n, end in enumerate(ends):
            if end == key:

                @pl.when(t != n)
                def _():
                    result(n, end)(n, t).start()

                @pl.when(t == n)
                def _():
                    own_copy(n).start()

    for tasks in rounds:
        for task in tasks:
            if task[0] == "coarse":
                _, n, source_key, target = task
                arrive(source_key)
                for i, p, r in pieces:
                    core, around = neighbours(reader(source_key), p, r)
                    field[slots[target], p + 1, pl.ds(r, step)] = core + piece(scale, p, r) * (
                        around - 6.0 * core + piece(forcing.at[n], p, r)
                    )
                    if i == 0 and r + step == window:
                        send(target, (0,))
            else:
                _, n, source_key, target, j, pair = task
                held = source_key[0] % 2 * slices + n
                arrive(source_key)
                if pair is not None:
                    arrive(pair[0])
                    arrive(pair[1])
                for i, p, r in pieces:
                    core, around = neighbours(reader(source_key), p, r)
                    gain = piece(inv, p, r)
                    if j == 1:
                        constant = core - gain * (6.0 * step_fine * core - step_fine * piece(forcing.at[n], p, r))
                        base[held, p, pl.ds(r, step)] = constant
                    else:
                        constant = piece(base.at[held], p, r)
                    value = constant + step_fine * gain * around
                    if pair is not None:
                        change, spread = neighbours(difference(*pair), p, r)
                        value = value + change + piece(scale, p, r) * (spread - 6.0 * change)
                    field[slots[target], p + 1, pl.ds(r, step)] = value
                    if i == 0 and r + step == window:
                        send(target, (0,))
            send(target, (1,))
            emit(target)

    for key in sorted(sent):
        arrive(key)
        for side, there in ((0, low_there), (1, high_there)):

            @pl.when(there)
            def _():
                halo(key, side).wait_send()

    for copy in ctrl_copies:
        copy.wait_send()
    for n in range(slices):

        @pl.when(t != n)
        def _():
            result(n, ends[n])(n, t).wait_send()
            result(n, ends[n])(t, n).wait_recv()

        @pl.when(t == n)
        def _():
            own_copy(n).wait()


def wide_kernel(size, state_hbm, cap_hbm, src_hbm, ctrl_ref, seg_ref, out_hbm,
                stage, given, inv, scale, bounds, coarse, sweep, base, near, change, state, end,
                seg_all, ctrl_all, load_sem, own_sem, in_send, in_recv, seg_send, seg_recv,
                ctrl_send, ctrl_recv, side_send, side_recv, mid_send, mid_recv,
                out_send, out_recv, last_sem):
    planes, rows, cols, slices, count, own = size
    total = planes * count
    devices = slices * count
    window = 3 * own
    mine = pl.ds(own, own)
    whole = pl.ds(1, total)
    t = lax.axis_index("tm")
    s = lax.axis_index("space")

    def swap(x):
        return x + x % 4 // 2 * (1 - 2 * (x % 2))

    def turn(x, level):
        return x + level % 2 * (slices - 1 - 2 * x)

    def index(t, s):
        chip = s // 2 * slices + turn(swap(t), s // 2)
        return 2 * chip + (s + chip) % 2

    def place(i):
        chip = i // 2
        level = chip // slices
        return swap(turn(chip % slices, level)), 2 * level + (i + chip) % 2

    here = index(t, s)
    has_low, has_high = here > 0, here < devices - 1

    def block(i):
        return pl.ds(pl.multiple_of(i * own, own), own)

    inputs = (state_hbm, cap_hbm, src_hbm)
    order = (1, 0, 2)
    loads = [pltpu.make_async_copy(inputs[a], stage.at[a], load_sem.at[a]) for a in range(3)]
    owns = [
        pltpu.make_async_copy(
            inputs[a].at[:, block(here)], given.at[a, pl.ds(1 + planes * s, planes), mine], own_sem.at[a]
        )
        for a in range(3)
    ]
    for a in order:
        loads[a].start()
    for a in order:
        owns[a].start()
    own_seg = pltpu.make_async_copy(seg_ref, seg_all.at[s], own_sem.at[3])
    own_ctrl = pltpu.make_async_copy(ctrl_ref, ctrl_all.at[0], own_sem.at[4])

    seg_all[...] = jnp.zeros(seg_all.shape, jnp.int32)
    barrier = pltpu.get_barrier_semaphore()
    for hop in range(1, count):
        pl.semaphore_signal(barrier, inc=1, device_id={"space": lax.rem(s + hop, count)})
    for hop in range(1, slices):
        pl.semaphore_signal(barrier, inc=1, device_id={"tm": lax.rem(t + hop, slices)})

    flat = jnp.zeros((window, cols), jnp.float32)
    for plane in (0, total + 1):
        given[0, plane] = flat
        for ref in (coarse, sweep, near, change, state, end):
            for k in range(ref.shape[0]):
                ref[k, plane] = flat
    for missing, at in ((has_low, 0), (has_high, 2 * own)):

        @pl.when(jnp.logical_not(missing))
        def _():
            side = jnp.zeros((total, own, cols), jnp.float32)
            given[0, whole, pl.ds(at, own)] = side
            given[1, whole, pl.ds(at, own)] = side + 1.0
            given[2, whole, pl.ds(at, own)] = side
            for k in range(state.shape[0]):
                state[k, whole, pl.ds(at, own)] = side

    pl.semaphore_wait(barrier, slices + count - 2)

    def spread(a, target, source):
        return pltpu.make_async_remote_copy(
            src_ref=stage.at[a, :, block(index(t, target))],
            dst_ref=given.at[a, pl.ds(1 + planes * source, planes), mine],
            send_sem=in_send.at[a, target],
            recv_sem=in_recv.at[a, source],
            device_id={"space": target},
        )

    def spread_seg(target, source):
        return pltpu.make_async_remote_copy(
            src_ref=seg_ref,
            dst_ref=seg_all.at[source],
            send_sem=seg_send.at[target],
            recv_sem=seg_recv.at[source],
            device_id={"space": target},
        )

    def side(make, send_sem, recv_sem, upward):
        other_t, other_s = place(here + 1 if upward else here - 1)
        return pltpu.make_async_remote_copy(
            src_ref=make(own),
            dst_ref=make(0 if upward else 2 * own),
            send_sem=send_sem.at[int(upward)],
            recv_sem=recv_sem.at[int(upward)],
            device_id={"tm": other_t, "space": other_s},
        )

    def side_start(*args):
        for upward, there in ((False, has_low), (True, has_high)):

            @pl.when(there)
            def _():
                side(*args, upward).start()

    def side_recv_wait(*args):
        for upward, there in ((True, has_low), (False, has_high)):

            @pl.when(there)
            def _():
                side(*args, upward).wait_recv()

    def side_send_wait(*args):
        for upward, there in ((False, has_low), (True, has_high)):

            @pl.when(there)
            def _():
                side(*args, upward).wait_send()

    def given_side(a):
        return lambda at: given.at[a, whole, pl.ds(at, own)], side_send.at[a], side_recv.at[a]

    def state_side(n):
        return lambda at: state.at[n - 1, whole, pl.ds(at, own)], mid_send.at[n - 1], mid_recv.at[n - 1]

    for a in order:
        loads[a].wait()
        for hop in range(1, count):
            target = lax.rem(s + hop, count)
            spread(a, target, s).start()
        if a == order[0]:
            own_seg.start()
            own_ctrl.start()
            ctrl_copies = []
            for hop in range(1, slices):
                ctrl_copies.append(pltpu.make_async_remote_copy(
                    src_ref=ctrl_ref,
                    dst_ref=ctrl_all.at[hop],
                    send_sem=ctrl_send.at[hop],
                    recv_sem=ctrl_recv.at[hop],
                    device_id={"tm": lax.rem(t + hop, slices)},
                ))
                ctrl_copies[-1].start()
            for target in (0, 1):

                @pl.when(jnp.logical_and(t == 0, s != target))
                def _():
                    spread_seg(target, s).start()

    row_id = lax.broadcasted_iota(jnp.int32, (window, cols), 0) + (here - 1) * own
    inside = jnp.logical_and(row_id >= 0, row_id < rows)
    step = planes
    spans = [pl.ds(p, step) for p in range(0, total, step)]

    def collect(a):
        owns[a].wait()
        for hop in range(1, count):
            source = lax.rem(s + count - hop, count)
            spread(a, s, source).wait_recv()
        side_start(*given_side(a))

    collect(1)
    collect(0)
    side_recv_wait(*given_side(1))
    for p in range(0, total, step):
        capacity = given[1, pl.ds(p + 1, step)]
        scale[pl.ds(p, step)] = jnp.where(inside, step_coarse / capacity, 0.0)
        inv[pl.ds(p, step)] = jnp.where(inside, 1.0 / (capacity + 6.0 * step_fine), 0.0)

    own_seg.wait()
    own_ctrl.wait()
    for copy in ctrl_copies:
        copy.wait_recv()
    for target in (0, 1):

        @pl.when(jnp.logical_and(t == 0, s == target))
        def _():
            for hop in range(1, count):
                source = (target + hop) % count
                spread_seg(target, source).wait_recv()

    segments = ctrl_ref.shape[1]
    for n in range(slices):
        row = jnp.zeros((1, segments), jnp.float32)
        for hop in range(slices):
            row = jnp.where(lax.rem(t - n + slices, slices) == hop, ctrl_all[hop], row)
        for source in range(count):
            segment = seg_all[source]
            values = jnp.zeros((planes, cols), jnp.float32)
            for k in range(segments):
                values = jnp.where(segment == k, row[:, k:k + 1], values)
            bounds[n, pl.ds(source * planes, planes)] = values

    collect(2)
    side_recv_wait(*given_side(0))
    side_recv_wait(*given_side(2))

    half = cols // 2
    lane = lax.broadcasted_iota(jnp.int32, (step, window, half), 2)
    first_row = row_id == 0

    def around(ref, p):
        core = ref[pl.ds(p + 1, step)]
        result = ref[pl.ds(p, step)] + ref[pl.ds(p + 2, step)]
        result = result + (pltpu.roll(core, 1, 1) + pltpu.roll(core, window - 1, 1))
        left, right = core[:, :, :half], core[:, :, half:]
        left_up, right_up = pltpu.roll(left, 1, 2), pltpu.roll(right, 1, 2)
        left_down, right_down = pltpu.roll(left, half - 1, 2), pltpu.roll(right, half - 1, 2)
        low = jnp.where(lane == 0, 0.0, left_up) + jnp.where(lane == half - 1, right_down, left_down)
        high = jnp.where(lane == 0, left_up, right_up) + jnp.where(lane == half - 1, 0.0, right_down)
        return core, result + jnp.concatenate([low, high], axis=2)

    def forcing(n, p):
        edge = bounds[n, pl.ds(p, step)][:, None, :]
        return given[2, pl.ds(p + 1, step)] + jnp.where(first_row[None], edge, 0.0)

    def begin(start, n, target, hold, ahead=None):
        for p in range(0, total, step):
            core, spread_sum = around(start, p)
            gain = inv[pl.ds(p, step)]
            drive = forcing(n, p) - 6.0 * step_fine * core
            constant = core + gain * drive
            hold[pl.ds(p, step)] = constant
            target[pl.ds(p + 1, step)] = constant + gain * spread_sum
            if ahead is not None:
                ahead[pl.ds(p + 1, step)] = core + scale[pl.ds(p, step)] * (drive + spread_sum)

    def go_on(source, hold, target):
        for p in range(0, total, step):
            _, spread_sum = around(source, p)
            target[pl.ds(p + 1, step)] = hold[pl.ds(p, step)] + inv[pl.ds(p, step)] * spread_sum

    def finish(source, hold, pair, keeps, only=()):
        if pair is not None:
            new, old, moved = pair
            for p in range(0, total, step):
                moved[pl.ds(p + 1, step)] = new[pl.ds(p + 1, step)] - old[pl.ds(p + 1, step)]
        for p in range(0, total, step):
            _, spread_sum = around(source, p)
            value = hold[pl.ds(p, step)] + inv[pl.ds(p, step)] * spread_sum
            if pair is not None:
                core, spread_sum = around(moved, p)
                value = value + (core + scale[pl.ds(p, step)] * (spread_sum - 6.0 * core))
            for ref in keeps:
                ref[pl.ds(p + 1, step)] = value
            for ref in only:
                ref[pl.ds(p + 1, step), mine] = value[:, own:2 * own]

    def solve(number, start, n, ahead, pair, keeps, only=()):
        a, b, hold = sweep.at[2 * number], sweep.at[2 * number + 1], base.at[number]
        begin(start, n, a, hold, ahead)
        for _ in range(SWEEPS - 2):
            go_on(a, hold, b)
            a, b = b, a
        finish(a, hold, pair, keeps, only)

    def deliver(n, target_s, source_t, source_s, ref):
        return pltpu.make_async_remote_copy(
            src_ref=ref.at[pl.ds(1 + planes * target_s, planes), mine],
            dst_ref=out_hbm.at[0, :, block(index(source_t, source_s))],
            send_sem=out_send.at[n, target_s],
            recv_sem=out_recv.at[source_t, source_s],
            device_id={"tm": n, "space": target_s},
        )

    def keep_local(n):
        return pltpu.make_async_copy(
            result[n].at[pl.ds(1 + planes * s, planes), mine], out_hbm.at[0, :, block(here)], last_sem.at[0]
        )

    result = [state.at[0]] + [end.at[n - 1] for n in range(1, slices)]

    def emit(n):
        for hop in range(1, count):
            deliver(n, lax.rem(s + hop, count), t, s, result[n]).start()

        @pl.when(t != n)
        def _():
            deliver(n, s, t, s, result[n]).start()

        @pl.when(t == n)
        def _():
            keep_local(n).start()

    starts = [given.at[0]] + [coarse.at[n - 1] for n in range(1, slices - 1)]
    for n in range(slices - 1):
        ahead = coarse.at[n] if n + 1 < slices - 1 else None
        pair = (near.at[n - 1], starts[n], change.at[n - 1]) if n else None
        keeps = (near.at[n],) if n + 1 < slices - 1 else ()
        solve(n, starts[n], n, ahead, pair, keeps, (state.at[n],))
        side_start(*state_side(n + 1))
        if n == 0:
            emit(0)
    for n in range(1, slices):
        side_recv_wait(*state_side(n))
        pair = (end.at[n - 2], state.at[n - 1], change.at[slices + n - 4]) if n > 1 else None
        keeps = (end.at[n - 1],) if n + 1 < slices else ()
        only = () if n + 1 < slices else (end.at[n - 1],)
        solve(slices - 2 + n, state.at[n - 1], n, None, pair, keeps, only)
        emit(n)

    for a in range(3):
        for hop in range(1, count):
            spread(a, lax.rem(s + hop, count), s).wait_send()
        side_send_wait(*given_side(a))
    for copy in ctrl_copies:
        copy.wait_send()
    for target in (0, 1):

        @pl.when(jnp.logical_and(t == 0, s != target))
        def _():
            spread_seg(target, s).wait_send()

    for n in range(1, slices):
        side_send_wait(*state_side(n))
    for n in range(slices):
        for hop in range(1, count):
            deliver(n, lax.rem(s + hop, count), t, s, result[n]).wait_send()

        @pl.when(t != n)
        def _():
            deliver(n, s, t, s, result[n]).wait_send()

        @pl.when(t == n)
        def _():
            keep_local(n).wait()

    for hop_t in range(slices):
        for hop_s in range(count):
            if hop_t or hop_s:
                source_t, source_s = lax.rem(t + hop_t, slices), lax.rem(s + hop_s, count)
                deliver(t, s, source_t, source_s, result[0]).wait_recv()


def wide_fits(slices, count, rows):
    own = rows // (slices * count)
    ordered = slices % 4 in (0, 2) and slices < 8 and count % 2 == 0
    return ordered and CORRECTIONS == 2 and slices > 2 and own % 8 == 0 and own >= SWEEPS + slices - 2 \
        and rows == own * slices * count


def solution(mesh):
    slices, count = mesh.shape["tm"], mesh.shape["space"]
    plan = make_plan(slices)

    def wide(initial_state, capacity, source, control, segment_index):
        planes, rows, cols = initial_state.shape
        own = rows // (slices * count)
        total, window = planes * count, 3 * own
        size = (planes, rows, cols, slices, count, own)
        dma = pltpu.SemaphoreType.DMA

        def fields(number):
            return pltpu.VMEM((number, total + 2, window, cols), jnp.float32)

        return pl.pallas_call(
            functools.partial(wide_kernel, size),
            out_shape=jax.ShapeDtypeStruct((1, planes, rows, cols), jnp.float32),
            in_specs=[pl.BlockSpec(memory_space=pl.ANY)] * 3 + [pl.BlockSpec(memory_space=pltpu.VMEM)] * 2,
            out_specs=pl.BlockSpec(memory_space=pl.ANY),
            scratch_shapes=[
                pltpu.VMEM((3, planes, rows, cols), jnp.float32),
                fields(3),
                pltpu.VMEM((total, window, cols), jnp.float32),
                pltpu.VMEM((total, window, cols), jnp.float32),
                pltpu.VMEM((slices, total, cols), jnp.float32),
                fields(slices - 2),
                fields(4 * (slices - 1)),
                pltpu.VMEM((2 * (slices - 1), total, window, cols), jnp.float32),
                fields(slices - 2),
                fields(2 * (slices - 2)),
                fields(slices - 1),
                fields(slices - 1),
                pltpu.VMEM((count,) + segment_index.shape, jnp.int32),
                pltpu.VMEM((slices,) + control.shape, jnp.float32),
                dma((3,)),
                dma((5,)),
                dma((3, count)),
                dma((3, count)),
                dma((count,)),
                dma((count,)),
                dma((slices,)),
                dma((slices,)),
                dma((3, 2)),
                dma((3, 2)),
                dma((slices - 1, 2)),
                dma((slices - 1, 2)),
                dma((slices, count)),
                dma((slices, count)),
                dma((1,)),
            ],
            compiler_params=pltpu.CompilerParams(
                collective_id=0, has_side_effects=True, vmem_limit_bytes=67043328 - 1048576
            ),
        )(initial_state, capacity, source, control, segment_index)

    def on_device(initial_state, capacity, source, control, segment_index):
        planes, rows, cols = initial_state.shape
        if wide_fits(slices, count, rows):
            return wide(initial_state, capacity, source, control, segment_index)
        own_rows = rows // slices
        reach = -(-(CORRECTIONS * SWEEPS + slices - CORRECTIONS) // 8) * 8
        window = min(rows, own_rows + 2 * reach)
        fields = len(plan[0])
        size = (planes, window, own_rows, reach, rows, cols, slices, count)
        block = (planes, window, cols)
        dma = pltpu.SemaphoreType.DMA
        return pl.pallas_call(
            functools.partial(kernel, plan, size),
            out_shape=jax.ShapeDtypeStruct((1, planes, rows, cols), jnp.float32),
            in_specs=[pl.BlockSpec(memory_space=pl.ANY)] * 3 + [pl.BlockSpec(memory_space=pltpu.VMEM)] * 2,
            out_specs=pl.BlockSpec(memory_space=pl.ANY),
            scratch_shapes=[
                pltpu.VMEM((fields, planes + 2, window, cols), jnp.float32),
                pltpu.VMEM((slices,) + block, jnp.float32),
                pltpu.VMEM((2 * slices,) + block, jnp.float32),
                pltpu.VMEM(block, jnp.float32),
                pltpu.VMEM(block, jnp.float32),
                pltpu.VMEM(block, jnp.float32),
                pltpu.VMEM((slices,) + control.shape, jnp.float32),
                dma((fields, 2)),
                dma((fields, 2)),
                dma((3,)),
                dma((slices,)),
                dma((slices,)),
                dma((slices,)),
                dma((slices,)),
                dma((2,)),
            ],
            compiler_params=pltpu.CompilerParams(
                collective_id=0, has_side_effects=True, vmem_limit_bytes=67043328 - 1048576
            ),
        )(initial_state, capacity, source, control, segment_index)

    return jax.shard_map(
        on_device,
        mesh=mesh,
        in_specs=(
            P("space", None, None),
            P("space", None, None),
            P("space", None, None),
            P("tm", None),
            P("space", None),
        ),
        out_specs=P("tm", "space", None, None),
        check_vma=False,
    )
```

```python
import functools

import jax
import jax.numpy as jnp
from jax import lax
from jax.experimental import pallas as pl
from jax.experimental.pallas import tpu as pltpu
from jax.sharding import PartitionSpec as P

SWEEPS = 6
CORRECTIONS = 2
step_fine = 1.0
step_coarse = 0.08


def make_plan(slices):
    last = CORRECTIONS
    solves = [
        (k, n)
        for k in range(last)
        for n in range(k, slices)
        if k == last - 1 or n + 1 < slices or n == k
    ]
    slots, sent = {}, set()
    for k, n in solves:
        for j in range(SWEEPS):
            slots[(k, n, j)] = len(slots)
            sent.add((k, n, j))

    def state(k, n):
        k = min(k, n)
        key = (k, n, 0)
        if key not in slots:
            slots[key] = len(slots)
        return key

    ends = [state(last, n + 1) for n in range(slices)]
    rounds = {}
    top_coarse = max(n for k, n in solves if k == 0)
    for n in range(top_coarse):
        rounds.setdefault(n + 1, []).append(("coarse", n, state(0, n), state(0, n + 1)))
    for k, n in sorted(solves, key=lambda item: (-item[0], item[1])):
        begin = SWEEPS * k + n - k
        for j in range(1, SWEEPS + 1):
            target = (k, n, j) if j < SWEEPS else state(k + 1, n + 1)
            pair = None
            if j == SWEEPS and k < n:
                pair = (state(k + 1, n), state(k, n))
                sent.add(pair[0])
                sent.add(pair[1])
            rounds.setdefault(begin + j, []).append(("sweep", n, (k, n, j - 1), target, j, pair))
    return slots, sent, [rounds[r] for r in sorted(rounds)], ends


def kernel(plan, size, state_hbm, cap_hbm, src_hbm, ctrl_ref, seg_ref, out_hbm,
           field, forcing, base, inv, scale, source, ctrl_all,
           send_sem, recv_sem, in_sem, ctrl_send, ctrl_recv, out_send, out_recv, own_sem):
    slots, sent, rounds, ends = plan
    planes, window, own_rows, reach, rows, cols, slices, count = size
    t = lax.axis_index("tm")
    s = lax.axis_index("space")
    low_there, high_there = s > 0, s < count - 1
    first_row = pl.multiple_of(jnp.clip(t * own_rows - reach, 0, rows - window), 8)
    own_at = pl.multiple_of(t * own_rows - first_row, 8)
    inner = pl.ds(1, planes)
    first = slots[(0, 0, 0)]

    loads = []
    for index, (ref, target) in enumerate(
        ((state_hbm, field.at[first, inner]), (cap_hbm, inv), (src_hbm, source))
    ):
        loads.append(pltpu.make_async_copy(ref.at[:, pl.ds(first_row, window), :], target, in_sem.at[index]))
        loads[-1].start()

    @pl.when(jnp.logical_not(low_there))
    def _():
        for key in sorted(sent):
            field[slots[key], 0] = jnp.zeros((window, cols), jnp.float32)

    @pl.when(jnp.logical_not(high_there))
    def _():
        for key in sorted(sent):
            field[slots[key], planes + 1] = jnp.zeros((window, cols), jnp.float32)

    barrier = pltpu.get_barrier_semaphore()

    @pl.when(low_there)
    def _():
        pl.semaphore_signal(barrier, inc=1, device_id={"space": s - 1})

    @pl.when(high_there)
    def _():
        pl.semaphore_signal(barrier, inc=1, device_id={"space": s + 1})

    for hop in range(1, slices):
        pl.semaphore_signal(barrier, inc=1, device_id={"tm": lax.rem(t + hop, slices)})
    pl.semaphore_wait(barrier, slices - 1 + jnp.minimum(s, 1) + jnp.minimum(count - 1 - s, 1))

    def halo(key, side):
        slot = slots[key]
        if side == 0:
            source_plane, target_plane, other = 1, planes + 1, s - 1
        else:
            source_plane, target_plane, other = planes, 0, s + 1
        k, n, j = key
        left = CORRECTIONS * (SWEEPS - 1) + slices - (k * (SWEEPS - 1) + n + j)
        near = min(-(-left // 8) * 8, reach)
        height = min(window, own_rows + 2 * near)
        at = jnp.clip(t * own_rows - near, 0, rows - height) - first_row
        needed = pl.ds(pl.multiple_of(at, 8), height)
        return pltpu.make_async_remote_copy(
            src_ref=field.at[slot, source_plane, needed],
            dst_ref=field.at[slot, target_plane, needed],
            send_sem=send_sem.at[slot, side],
            recv_sem=recv_sem.at[slot, side],
            device_id={"space": other},
        )

    odd = lax.rem(s, 2)

    def send(key, parts=(0, 1)):
        if key in sent:
            for part in parts:
                for side, there in ((0, low_there), (1, high_there)):

                    @pl.when(jnp.logical_and(there, odd == (side + part) % 2))
                    def _():
                        halo(key, side).start()

    arrived = set()

    def arrive(key):
        if key in arrived:
            return
        arrived.add(key)
        for side, there in ((0, high_there), (1, low_there)):

            @pl.when(there)
            def _():
                halo(key, side).wait_recv()

    loads[0].wait()
    send((0, 0, 0))

    ctrl_copies = []
    for hop in range(1, slices):
        ctrl_copies.append(pltpu.make_async_remote_copy(
            src_ref=ctrl_ref,
            dst_ref=ctrl_all.at[hop],
            send_sem=ctrl_send.at[hop],
            recv_sem=ctrl_recv.at[hop],
            device_id={"tm": lax.rem(t + hop, slices)},
        ))
        ctrl_copies[-1].start()
    own_ctrl = pltpu.make_async_copy(ctrl_ref, ctrl_all.at[0], own_sem.at[0])
    own_ctrl.start()

    loads[1].wait()
    capacity = inv[...]
    scale[...] = step_coarse / capacity
    reciprocal = 1.0 / (capacity + 6.0 * step_fine)
    inv[...] = reciprocal
    loads[2].wait()
    own_ctrl.wait()
    for copy in ctrl_copies:
        copy.wait_recv()

    segment = seg_ref[...]
    segments = ctrl_ref.shape[1]
    row_id = lax.broadcasted_iota(jnp.int32, (planes, window, cols), 1) + first_row
    for n in range(slices):
        row = jnp.zeros((1, segments), jnp.float32)
        for hop in range(slices):
            row = jnp.where(lax.rem(t - n + slices, slices) == hop, ctrl_all[hop], row)
        values = jnp.zeros((planes, cols), jnp.float32)
        for k in range(segments):
            values = jnp.where(segment == k, row[:, k:k + 1], values)
        forcing[n] = source[...] + jnp.where(row_id == 0, values[:, None, :], 0.0)

    step = window // 2 if window % 16 == 0 else window
    lane = lax.broadcasted_iota(jnp.int32, (step, cols), 1)
    line = lax.broadcasted_iota(jnp.int32, (step, cols), 0)
    pieces = []
    for i in range(planes):
        p = jnp.where(odd == 1, planes - 1 - i, i)
        pieces += [(i, p, r) for r in range(0, window, step)]

    def neighbours(read, p, r):
        core = read(p + 1, r)
        if r > 0:
            above = read(p + 1, r - 1)
        else:
            above = jnp.where(line == 0, 0.0, pltpu.roll(core, 1, 0))
        if r + step < window:
            below = read(p + 1, r + 1)
        else:
            below = jnp.where(line == step - 1, 0.0, pltpu.roll(core, step - 1, 0))
        left = jnp.where(lane == 0, 0.0, pltpu.roll(core, 1, 1))
        right = jnp.where(lane == cols - 1, 0.0, pltpu.roll(core, cols - 1, 1))
        return core, read(p, r) + read(p + 2, r) + above + below + left + right

    def reader(key):
        return lambda p, r: field[slots[key], p, pl.ds(r, step)]

    def difference(new, old):
        return lambda p, r: field[slots[new], p, pl.ds(r, step)] - field[slots[old], p, pl.ds(r, step)]

    def piece(ref, p, r):
        return ref[p, pl.ds(r, step)]

    def result(n, end):
        def remote(target, source_slice):
            return pltpu.make_async_remote_copy(
                src_ref=field.at[slots[end], inner, pl.ds(own_at, own_rows)],
                dst_ref=out_hbm.at[0, :, pl.ds(pl.multiple_of(source_slice * own_rows, 8), own_rows)],
                send_sem=out_send.at[target],
                recv_sem=out_recv.at[source_slice],
                device_id={"tm": target},
            )
        return remote

    def own_copy(n):
        return pltpu.make_async_copy(
            field.at[slots[ends[n]], inner, pl.ds(own_at, own_rows)],
            out_hbm.at[0, :, pl.ds(n * own_rows, own_rows)],
            own_sem.at[1],
        )

    def emit(key):
        for n, end in enumerate(ends):
            if end == key:

                @pl.when(t != n)
                def _():
                    result(n, end)(n, t).start()

                @pl.when(t == n)
                def _():
                    own_copy(n).start()

    for tasks in rounds:
        for task in tasks:
            if task[0] == "coarse":
                _, n, source_key, target = task
                arrive(source_key)
                for i, p, r in pieces:
                    core, around = neighbours(reader(source_key), p, r)
                    field[slots[target], p + 1, pl.ds(r, step)] = core + piece(scale, p, r) * (
                        around - 6.0 * core + piece(forcing.at[n], p, r)
                    )
                    if i == 0 and r + step == window:
                        send(target, (0,))
            else:
                _, n, source_key, target, j, pair = task
                held = source_key[0] % 2 * slices + n
                arrive(source_key)
                if pair is not None:
                    arrive(pair[0])
                    arrive(pair[1])
                for i, p, r in pieces:
                    core, around = neighbours(reader(source_key), p, r)
                    gain = piece(inv, p, r)
                    if j == 1:
                        constant = core - gain * (6.0 * step_fine * core - step_fine * piece(forcing.at[n], p, r))
                        base[held, p, pl.ds(r, step)] = constant
                    else:
                        constant = piece(base.at[held], p, r)
                    value = constant + step_fine * gain * around
                    if pair is not None:
                        change, spread = neighbours(difference(*pair), p, r)
                        value = value + change + piece(scale, p, r) * (spread - 6.0 * change)
                    field[slots[target], p + 1, pl.ds(r, step)] = value
                    if i == 0 and r + step == window:
                        send(target, (0,))
            send(target, (1,))
            emit(target)

    for key in sorted(sent):
        arrive(key)
        for side, there in ((0, low_there), (1, high_there)):

            @pl.when(there)
            def _():
                halo(key, side).wait_send()

    for copy in ctrl_copies:
        copy.wait_send()
    for n in range(slices):

        @pl.when(t != n)
        def _():
            result(n, ends[n])(n, t).wait_send()
            result(n, ends[n])(t, n).wait_recv()

        @pl.when(t == n)
        def _():
            own_copy(n).wait()


def wide_kernel(size, state_hbm, cap_hbm, src_hbm, ctrl_ref, seg_ref, out_hbm,
                stage, given, inv, scale, bounds, coarse, sweep, base, near, change, state, end,
                seg_all, ctrl_all, load_sem, own_sem, in_send, in_recv, seg_send, seg_recv,
                ctrl_send, ctrl_recv, side_send, side_recv, mid_send, mid_recv,
                out_send, out_recv, last_sem):
    planes, rows, cols, slices, count, own = size
    total = planes * count
    devices = slices * count
    window, pad, lanes = 3 * own, 8, 128
    parts = cols // lanes
    mine = pl.ds(pad + own, own)
    whole = pl.ds(1, total)
    t = lax.axis_index("tm")
    s = lax.axis_index("space")

    def swap(x):
        return x + x % 4 // 2 * (1 - 2 * (x % 2))

    def turn(x, level):
        return x + level % 2 * (slices - 1 - 2 * x)

    def index(t, s):
        chip = s // 2 * slices + turn(swap(t), s // 2)
        return 2 * chip + (s + chip) % 2

    def place(i):
        chip = i // 2
        level = chip // slices
        return swap(turn(chip % slices, level)), 2 * level + (i + chip) % 2

    here = index(t, s)
    has_low, has_high = here > 0, here < devices - 1

    def block(i):
        return pl.ds(pl.multiple_of(i * own, own), own)

    inputs = (state_hbm, cap_hbm, src_hbm)
    order = (1, 0, 2)
    loads = [
        [
            pltpu.make_async_copy(
                inputs[a].at[:, :, pl.ds(h * lanes, lanes)], stage.at[a, :, h], load_sem.at[a, h]
            )
            for h in range(parts)
        ]
        for a in range(3)
    ]
    owns = [
        [
            pltpu.make_async_copy(
                inputs[a].at[:, block(here), pl.ds(h * lanes, lanes)],
                given.at[a, pl.ds(1 + planes * s, planes), h, mine],
                own_sem.at[a, h],
            )
            for h in range(parts)
        ]
        for a in range(3)
    ]
    for group in (loads, owns):
        for a in order:
            for copy in group[a]:
                copy.start()
    own_seg = pltpu.make_async_copy(seg_ref, seg_all.at[s], last_sem.at[1])
    own_ctrl = pltpu.make_async_copy(ctrl_ref, ctrl_all.at[0], last_sem.at[2])

    seg_all[...] = jnp.zeros(seg_all.shape, jnp.int32)
    barrier = pltpu.get_barrier_semaphore()
    for hop in range(1, count):
        pl.semaphore_signal(barrier, inc=1, device_id={"space": lax.rem(s + hop, count)})
    for hop in range(1, slices):
        pl.semaphore_signal(barrier, inc=1, device_id={"tm": lax.rem(t + hop, slices)})

    flat = jnp.zeros((parts, window + 2 * pad, lanes), jnp.float32)
    for plane in (0, total + 1):
        given[0, plane] = flat
        for ref in (coarse, sweep, change, state):
            for k in range(ref.shape[0]):
                ref[k, plane] = flat
    for missing, at in ((has_low, pad), (has_high, pad + 2 * own)):

        @pl.when(jnp.logical_not(missing))
        def _():
            side = jnp.zeros((total, parts, own, lanes), jnp.float32)
            given[0, whole, :, pl.ds(at, own)] = side
            given[1, whole, :, pl.ds(at, own)] = side + 1.0
            given[2, whole, :, pl.ds(at, own)] = side
            for k in range(state.shape[0]):
                state[k, whole, :, pl.ds(at, own)] = side

    pl.semaphore_wait(barrier, slices + count - 2)

    def spread(a, target, source):
        return pltpu.make_async_remote_copy(
            src_ref=stage.at[a, :, :, block(index(t, target))],
            dst_ref=given.at[a, pl.ds(1 + planes * source, planes), :, mine],
            send_sem=in_send.at[a, target],
            recv_sem=in_recv.at[a, source],
            device_id={"space": target},
        )

    def spread_seg(target, source):
        return pltpu.make_async_remote_copy(
            src_ref=seg_ref,
            dst_ref=seg_all.at[source],
            send_sem=seg_send.at[target],
            recv_sem=seg_recv.at[source],
            device_id={"space": target},
        )

    def side(origin, target, send_sem, recv_sem, upward):
        other_t, other_s = place(here + 1 if upward else here - 1)
        return pltpu.make_async_remote_copy(
            src_ref=origin.at[whole, :, mine],
            dst_ref=target.at[whole, :, pl.ds(pad if upward else pad + 2 * own, own)],
            send_sem=send_sem.at[int(upward)],
            recv_sem=recv_sem.at[int(upward)],
            device_id={"tm": other_t, "space": other_s},
        )

    def side_start(*args):
        for upward, there in ((False, has_low), (True, has_high)):

            @pl.when(there)
            def _():
                side(*args, upward).start()

    def side_recv_wait(*args):
        for upward, there in ((True, has_low), (False, has_high)):

            @pl.when(there)
            def _():
                side(*args, upward).wait_recv()

    def side_send_wait(*args):
        for upward, there in ((False, has_low), (True, has_high)):

            @pl.when(there)
            def _():
                side(*args, upward).wait_send()

    def given_side(a):
        return given.at[a], given.at[a], side_send.at[a], side_recv.at[a]

    def state_side(n):
        return near.at[n - 1], state.at[n - 1], mid_send.at[n - 1], mid_recv.at[n - 1]

    for a in order:
        for copy in loads[a]:
            copy.wait()
        for hop in range(1, count):
            target = lax.rem(s + hop, count)
            spread(a, target, s).start()
        if a == order[0]:
            own_seg.start()
            own_ctrl.start()
            ctrl_copies = []
            for hop in range(1, slices):
                ctrl_copies.append(pltpu.make_async_remote_copy(
                    src_ref=ctrl_ref,
                    dst_ref=ctrl_all.at[hop],
                    send_sem=ctrl_send.at[hop],
                    recv_sem=ctrl_recv.at[hop],
                    device_id={"tm": lax.rem(t + hop, slices)},
                ))
                ctrl_copies[-1].start()
            for target in (0, 1):

                @pl.when(jnp.logical_and(t == 0, s != target))
                def _():
                    spread_seg(target, s).start()

    step = 2
    row_id = lax.broadcasted_iota(jnp.int32, (step, parts, window, lanes), 2) + (here - 1) * own
    inside = jnp.logical_and(row_id >= 0, row_id < rows)
    all_rows = pl.ds(pad, window)

    def collect(a):
        for copy in owns[a]:
            copy.wait()
        for hop in range(1, count):
            source = lax.rem(s + count - hop, count)
            spread(a, s, source).wait_recv()
        side_start(*given_side(a))

    collect(1)
    collect(0)
    side_recv_wait(*given_side(1))
    for p in range(0, total, step):
        capacity = given[1, pl.ds(p + 1, step), :, all_rows]
        scale[pl.ds(p, step), :, all_rows] = jnp.where(inside, step_coarse / capacity, 0.0)
        inv[pl.ds(p, step), :, all_rows] = jnp.where(inside, 1.0 / (capacity + 6.0 * step_fine), 0.0)

    own_seg.wait()
    own_ctrl.wait()
    for copy in ctrl_copies:
        copy.wait_recv()
    for target in (0, 1):

        @pl.when(jnp.logical_and(t == 0, s == target))
        def _():
            for hop in range(1, count):
                source = (target + hop) % count
                spread_seg(target, source).wait_recv()

    segments = ctrl_ref.shape[1]
    for n in range(slices):
        row = jnp.zeros((1, segments), jnp.float32)
        for hop in range(slices):
            row = jnp.where(lax.rem(t - n + slices, slices) == hop, ctrl_all[hop], row)
        for source in range(count):
            segment = seg_all[source]
            values = jnp.zeros((planes, cols), jnp.float32)
            for k in range(segments):
                values = jnp.where(segment == k, row[:, k:k + 1], values)
            for plane in range(planes):
                for h in range(parts):
                    bounds[n, source * planes + plane, h] = jnp.broadcast_to(
                        values[plane:plane + 1, h * lanes:(h + 1) * lanes], (8, lanes)
                    )

    collect(2)
    side_recv_wait(*given_side(0))
    side_recv_wait(*given_side(2))

    lane = lax.broadcasted_iota(jnp.int32, (step, 8, lanes), 2)
    lane_low, lane_high = lane == 0, lane == lanes - 1

    def extent(reach):
        extra = -(-reach // 4) * 4
        return own - extra, own + 2 * extra

    def load(ref, p, h, at, height):
        return ref[pl.ds(p, step), h, pl.ds(pad + at, height)]

    def rotate(value, amount):
        return pltpu.roll(value, amount % lanes, 2)

    def around(ref, p, at, height):
        cores, sums = [], []
        for h in range(parts):
            block = ref[pl.ds(p, step + 2), h, pl.ds(pad + at, height)]
            cores.append(block[1:step + 1])
            sums.append(block[:step] + block[2:] + (
                load(ref, p + 1, h, at - 1, height) + load(ref, p + 1, h, at + 1, height)
            ))
        ups = [rotate(core, 1) for core in cores]
        downs = [rotate(core, -1) for core in cores]
        low = jnp.concatenate([lane_low] * (height // 8), axis=1)
        high = jnp.concatenate([lane_high] * (height // 8), axis=1)
        for h in range(parts):
            left = jnp.where(low, ups[h - 1] if h else 0.0, ups[h])
            right = jnp.where(high, downs[h + 1] if h + 1 < parts else 0.0, downs[h])
            sums[h] = sums[h] + (left + right)
        return cores, sums

    def row_mask(at, height):
        row_id = lax.broadcasted_iota(jnp.int32, (step, height, lanes), 1) + ((here - 1) * own + at)
        return row_id == 0

    def begin(start, n, target, hold, ahead, reach):
        at, height = extent(reach)
        first_row = row_mask(at, height)
        for p in range(0, total, step):
            cores, sums = around(start, p, at, height)
            for h in range(parts):
                edge = jnp.concatenate([bounds[n, pl.ds(p, step), h]] * (height // 8), axis=1)
                gain = load(inv, p, h, at, height)
                drive = load(given.at[2], p + 1, h, at, height) + jnp.where(first_row, edge, 0.0)
                drive = drive - 6.0 * step_fine * cores[h]
                constant = cores[h] + gain * drive
                hold[pl.ds(p, step), h, pl.ds(pad + at, height)] = constant
                target[pl.ds(p + 1, step), h, pl.ds(pad + at, height)] = constant + gain * sums[h]
                if ahead is not None:
                    ahead[pl.ds(p + 1, step), h, pl.ds(pad + at, height)] = cores[h] + load(
                        scale, p, h, at, height
                    ) * (drive + sums[h])

    def go_on(source, hold, target, reach):
        at, height = extent(reach)
        for p in range(0, total, step):
            _, sums = around(source, p, at, height)
            for h in range(parts):
                target[pl.ds(p + 1, step), h, pl.ds(pad + at, height)] = load(
                    hold, p, h, at, height
                ) + load(inv, p, h, at, height) * sums[h]

    def finish(source, hold, pair, target, reach):
        if pair is not None:
            new, old, moved = pair
            at, height = extent(reach + 1)
            for p in range(0, total, step):
                for h in range(parts):
                    moved[pl.ds(p + 1, step), h, pl.ds(pad + at, height)] = load(
                        new, p + 1, h, at, height
                    ) - load(old, p + 1, h, at, height)
        at, height = extent(reach)
        for p in range(0, total, step):
            _, sums = around(source, p, at, height)
            if pair is not None:
                cores, spreads = around(moved, p, at, height)
            for h in range(parts):
                value = load(hold, p, h, at, height) + load(inv, p, h, at, height) * sums[h]
                if pair is not None:
                    value = value + (cores[h] + load(scale, p, h, at, height) * (spreads[h] - 6.0 * cores[h]))
                target[pl.ds(p + 1, step), h, pl.ds(pad + at, height)] = value

    def solve(number, start, n, ahead, pair, target, reach):
        a, b, hold = sweep.at[2 * number], sweep.at[2 * number + 1], base.at[number]
        begin(start, n, a, hold, ahead, reach + SWEEPS - 1)
        for j in range(2, SWEEPS):
            go_on(a, hold, b, reach + SWEEPS - j)
            a, b = b, a
        finish(a, hold, pair, target, reach)

    def deliver(n, target_s, source_t, source_s, ref):
        return pltpu.make_async_remote_copy(
            src_ref=ref.at[pl.ds(1 + planes * target_s, planes), :, mine],
            dst_ref=out_hbm.at[:, index(source_t, source_s)],
            send_sem=out_send.at[n, target_s],
            recv_sem=out_recv.at[source_t, source_s],
            device_id={"tm": n, "space": target_s},
        )

    def keep_local(n):
        return pltpu.make_async_copy(
            result[n].at[pl.ds(1 + planes * s, planes), :, mine], out_hbm.at[:, here], last_sem.at[0]
        )

    result = [near.at[0]] + [end.at[n - 1] for n in range(1, slices)]

    def emit(n):
        for hop in range(1, count):
            deliver(n, lax.rem(s + hop, count), t, s, result[n]).start()

        @pl.when(t != n)
        def _():
            deliver(n, s, t, s, result[n]).start()

        @pl.when(t == n)
        def _():
            keep_local(n).start()

    starts = [given.at[0]] + [coarse.at[n - 1] for n in range(1, slices - 1)]
    for n in range(slices - 1):
        ahead = coarse.at[n] if n + 2 < slices else None
        pair = (near.at[n - 1], starts[n], change.at[n - 1]) if n else None
        solve(n, starts[n], n, ahead, pair, near.at[n], slices - 2 - n)
        side_start(*state_side(n + 1))
        if n == 0:
            emit(0)
        for p in range(0, total, step):
            state[n, pl.ds(p + 1, step), :, mine] = near[n, pl.ds(p + 1, step), :, mine]
    for n in range(1, slices):
        side_recv_wait(*state_side(n))
        pair = (end.at[n - 2], state.at[n - 1], change.at[slices + n - 4]) if n > 1 else None
        solve(slices - 2 + n, state.at[n - 1], n, None, pair, end.at[n - 1], slices - 1 - n)
        emit(n)

    for a in range(3):
        for hop in range(1, count):
            spread(a, lax.rem(s + hop, count), s).wait_send()
        side_send_wait(*given_side(a))
    for copy in ctrl_copies:
        copy.wait_send()
    for target in (0, 1):

        @pl.when(jnp.logical_and(t == 0, s != target))
        def _():
            spread_seg(target, s).wait_send()

    for n in range(1, slices):
        side_send_wait(*state_side(n))
    for n in range(slices):
        for hop in range(1, count):
            deliver(n, lax.rem(s + hop, count), t, s, result[n]).wait_send()

        @pl.when(t != n)
        def _():
            deliver(n, s, t, s, result[n]).wait_send()

        @pl.when(t == n)
        def _():
            keep_local(n).wait()

    for hop_t in range(slices):
        for hop_s in range(count):
            if hop_t or hop_s:
                source_t, source_s = lax.rem(t + hop_t, slices), lax.rem(s + hop_s, count)
                deliver(t, s, source_t, source_s, result[0]).wait_recv()


def wide_fits(slices, count, rows, cols):
    own = rows // (slices * count)
    ordered = slices % 4 in (0, 2) and slices < 8 and count % 2 == 0
    return ordered and CORRECTIONS == 2 and slices > 2 and own == 8 and own >= SWEEPS + slices - 2 \
        and rows == own * slices * count and cols % 128 == 0


def solution(mesh):
    slices, count = mesh.shape["tm"], mesh.shape["space"]
    plan = make_plan(slices)

    def wide(initial_state, capacity, source, control, segment_index):
        planes, rows, cols = initial_state.shape
        own = rows // (slices * count)
        total, window, parts = planes * count, 3 * own, cols // 128
        still = (total, parts, window + 16, 128)
        size = (planes, rows, cols, slices, count, own)
        dma = pltpu.SemaphoreType.DMA

        def fields(number):
            return pltpu.VMEM((number, total + 2, parts, window + 16, 128), jnp.float32)

        result = pl.pallas_call(
            functools.partial(wide_kernel, size),
            out_shape=jax.ShapeDtypeStruct((planes, rows // own, parts, own, 128), jnp.float32),
            in_specs=[pl.BlockSpec(memory_space=pl.ANY)] * 3 + [pl.BlockSpec(memory_space=pltpu.VMEM)] * 2,
            out_specs=pl.BlockSpec(memory_space=pl.ANY),
            scratch_shapes=[
                pltpu.VMEM((3, planes, parts, rows, 128), jnp.float32),
                fields(3),
                pltpu.VMEM(still, jnp.float32),
                pltpu.VMEM(still, jnp.float32),
                pltpu.VMEM((slices, total, parts, 8, 128), jnp.float32),
                fields(slices - 2),
                fields(4 * (slices - 1)),
                pltpu.VMEM((2 * (slices - 1),) + still, jnp.float32),
                fields(slices - 1),
                fields(2 * (slices - 2)),
                fields(slices - 1),
                fields(slices - 1),
                pltpu.VMEM((count,) + segment_index.shape, jnp.int32),
                pltpu.VMEM((slices,) + control.shape, jnp.float32),
                dma((3, parts)),
                dma((3, parts)),
                dma((3, count)),
                dma((3, count)),
                dma((count,)),
                dma((count,)),
                dma((slices,)),
                dma((slices,)),
                dma((3, 2)),
                dma((3, 2)),
                dma((slices - 1, 2)),
                dma((slices - 1, 2)),
                dma((slices, count)),
                dma((slices, count)),
                dma((3,)),
            ],
            compiler_params=pltpu.CompilerParams(
                collective_id=0, has_side_effects=True, vmem_limit_bytes=67043328 - 1048576
            ),
        )(initial_state, capacity, source, control, segment_index)
        return result.transpose(0, 1, 3, 2, 4).reshape(1, planes, rows, cols)

    def on_device(initial_state, capacity, source, control, segment_index):
        planes, rows, cols = initial_state.shape
        if wide_fits(slices, count, rows, cols):
            return wide(initial_state, capacity, source, control, segment_index)
        own_rows = rows // slices
        reach = -(-(CORRECTIONS * SWEEPS + slices - CORRECTIONS) // 8) * 8
        window = min(rows, own_rows + 2 * reach)
        fields = len(plan[0])
        size = (planes, window, own_rows, reach, rows, cols, slices, count)
        block = (planes, window, cols)
        dma = pltpu.SemaphoreType.DMA
        return pl.pallas_call(
            functools.partial(kernel, plan, size),
            out_shape=jax.ShapeDtypeStruct((1, planes, rows, cols), jnp.float32),
            in_specs=[pl.BlockSpec(memory_space=pl.ANY)] * 3 + [pl.BlockSpec(memory_space=pltpu.VMEM)] * 2,
            out_specs=pl.BlockSpec(memory_space=pl.ANY),
            scratch_shapes=[
                pltpu.VMEM((fields, planes + 2, window, cols), jnp.float32),
                pltpu.VMEM((slices,) + block, jnp.float32),
                pltpu.VMEM((2 * slices,) + block, jnp.float32),
                pltpu.VMEM(block, jnp.float32),
                pltpu.VMEM(block, jnp.float32),
                pltpu.VMEM(block, jnp.float32),
                pltpu.VMEM((slices,) + control.shape, jnp.float32),
                dma((fields, 2)),
                dma((fields, 2)),
                dma((3,)),
                dma((slices,)),
                dma((slices,)),
                dma((slices,)),
                dma((slices,)),
                dma((2,)),
            ],
            compiler_params=pltpu.CompilerParams(
                collective_id=0, has_side_effects=True, vmem_limit_bytes=67043328 - 1048576
            ),
        )(initial_state, capacity, source, control, segment_index)

    return jax.shard_map(
        on_device,
        mesh=mesh,
        in_specs=(
            P("space", None, None),
            P("space", None, None),
            P("space", None, None),
            P("tm", None),
            P("space", None),
        ),
        out_specs=P("tm", "space", None, None),
        check_vma=False,
    )
```

```python
import functools

import jax
import jax.numpy as jnp
from jax import lax
from jax.experimental import pallas as pl
from jax.experimental.pallas import tpu as pltpu
from jax.sharding import PartitionSpec as P

SWEEPS = 6
CORRECTIONS = 2
step_fine = 1.0
step_coarse = 0.08


def make_plan(slices):
    last = CORRECTIONS
    solves = [
        (k, n)
        for k in range(last)
        for n in range(k, slices)
        if k == last - 1 or n + 1 < slices or n == k
    ]
    slots, sent = {}, set()
    for k, n in solves:
        for j in range(SWEEPS):
            slots[(k, n, j)] = len(slots)
            sent.add((k, n, j))

    def state(k, n):
        k = min(k, n)
        key = (k, n, 0)
        if key not in slots:
            slots[key] = len(slots)
        return key

    ends = [state(last, n + 1) for n in range(slices)]
    rounds = {}
    top_coarse = max(n for k, n in solves if k == 0)
    for n in range(top_coarse):
        rounds.setdefault(n + 1, []).append(("coarse", n, state(0, n), state(0, n + 1)))
    for k, n in sorted(solves, key=lambda item: (-item[0], item[1])):
        begin = SWEEPS * k + n - k
        for j in range(1, SWEEPS + 1):
            target = (k, n, j) if j < SWEEPS else state(k + 1, n + 1)
            pair = None
            if j == SWEEPS and k < n:
                pair = (state(k + 1, n), state(k, n))
                sent.add(pair[0])
                sent.add(pair[1])
            rounds.setdefault(begin + j, []).append(("sweep", n, (k, n, j - 1), target, j, pair))
    return slots, sent, [rounds[r] for r in sorted(rounds)], ends


def kernel(plan, size, state_hbm, cap_hbm, src_hbm, ctrl_ref, seg_ref, out_hbm,
           field, forcing, base, inv, scale, source, ctrl_all,
           send_sem, recv_sem, in_sem, ctrl_send, ctrl_recv, out_send, out_recv, own_sem):
    slots, sent, rounds, ends = plan
    planes, window, own_rows, reach, rows, cols, slices, count = size
    t = lax.axis_index("tm")
    s = lax.axis_index("space")
    low_there, high_there = s > 0, s < count - 1
    first_row = pl.multiple_of(jnp.clip(t * own_rows - reach, 0, rows - window), 8)
    own_at = pl.multiple_of(t * own_rows - first_row, 8)
    inner = pl.ds(1, planes)
    first = slots[(0, 0, 0)]

    loads = []
    for index, (ref, target) in enumerate(
        ((state_hbm, field.at[first, inner]), (cap_hbm, inv), (src_hbm, source))
    ):
        loads.append(pltpu.make_async_copy(ref.at[:, pl.ds(first_row, window), :], target, in_sem.at[index]))
        loads[-1].start()

    @pl.when(jnp.logical_not(low_there))
    def _():
        for key in sorted(sent):
            field[slots[key], 0] = jnp.zeros((window, cols), jnp.float32)

    @pl.when(jnp.logical_not(high_there))
    def _():
        for key in sorted(sent):
            field[slots[key], planes + 1] = jnp.zeros((window, cols), jnp.float32)

    barrier = pltpu.get_barrier_semaphore()

    @pl.when(low_there)
    def _():
        pl.semaphore_signal(barrier, inc=1, device_id={"space": s - 1})

    @pl.when(high_there)
    def _():
        pl.semaphore_signal(barrier, inc=1, device_id={"space": s + 1})

    for hop in range(1, slices):
        pl.semaphore_signal(barrier, inc=1, device_id={"tm": lax.rem(t + hop, slices)})
    pl.semaphore_wait(barrier, slices - 1 + jnp.minimum(s, 1) + jnp.minimum(count - 1 - s, 1))

    def halo(key, side):
        slot = slots[key]
        if side == 0:
            source_plane, target_plane, other = 1, planes + 1, s - 1
        else:
            source_plane, target_plane, other = planes, 0, s + 1
        k, n, j = key
        left = CORRECTIONS * (SWEEPS - 1) + slices - (k * (SWEEPS - 1) + n + j)
        near = min(-(-left // 8) * 8, reach)
        height = min(window, own_rows + 2 * near)
        at = jnp.clip(t * own_rows - near, 0, rows - height) - first_row
        needed = pl.ds(pl.multiple_of(at, 8), height)
        return pltpu.make_async_remote_copy(
            src_ref=field.at[slot, source_plane, needed],
            dst_ref=field.at[slot, target_plane, needed],
            send_sem=send_sem.at[slot, side],
            recv_sem=recv_sem.at[slot, side],
            device_id={"space": other},
        )

    odd = lax.rem(s, 2)

    def send(key, parts=(0, 1)):
        if key in sent:
            for part in parts:
                for side, there in ((0, low_there), (1, high_there)):

                    @pl.when(jnp.logical_and(there, odd == (side + part) % 2))
                    def _():
                        halo(key, side).start()

    arrived = set()

    def arrive(key):
        if key in arrived:
            return
        arrived.add(key)
        for side, there in ((0, high_there), (1, low_there)):

            @pl.when(there)
            def _():
                halo(key, side).wait_recv()

    loads[0].wait()
    send((0, 0, 0))

    ctrl_copies = []
    for hop in range(1, slices):
        ctrl_copies.append(pltpu.make_async_remote_copy(
            src_ref=ctrl_ref,
            dst_ref=ctrl_all.at[hop],
            send_sem=ctrl_send.at[hop],
            recv_sem=ctrl_recv.at[hop],
            device_id={"tm": lax.rem(t + hop, slices)},
        ))
        ctrl_copies[-1].start()
    own_ctrl = pltpu.make_async_copy(ctrl_ref, ctrl_all.at[0], own_sem.at[0])
    own_ctrl.start()

    loads[1].wait()
    capacity = inv[...]
    scale[...] = step_coarse / capacity
    reciprocal = 1.0 / (capacity + 6.0 * step_fine)
    inv[...] = reciprocal
    loads[2].wait()
    own_ctrl.wait()
    for copy in ctrl_copies:
        copy.wait_recv()

    segment = seg_ref[...]
    segments = ctrl_ref.shape[1]
    row_id = lax.broadcasted_iota(jnp.int32, (planes, window, cols), 1) + first_row
    for n in range(slices):
        row = jnp.zeros((1, segments), jnp.float32)
        for hop in range(slices):
            row = jnp.where(lax.rem(t - n + slices, slices) == hop, ctrl_all[hop], row)
        values = jnp.zeros((planes, cols), jnp.float32)
        for k in range(segments):
            values = jnp.where(segment == k, row[:, k:k + 1], values)
        forcing[n] = source[...] + jnp.where(row_id == 0, values[:, None, :], 0.0)

    step = window // 2 if window % 16 == 0 else window
    lane = lax.broadcasted_iota(jnp.int32, (step, cols), 1)
    line = lax.broadcasted_iota(jnp.int32, (step, cols), 0)
    pieces = []
    for i in range(planes):
        p = jnp.where(odd == 1, planes - 1 - i, i)
        pieces += [(i, p, r) for r in range(0, window, step)]

    def neighbours(read, p, r):
        core = read(p + 1, r)
        if r > 0:
            above = read(p + 1, r - 1)
        else:
            above = jnp.where(line == 0, 0.0, pltpu.roll(core, 1, 0))
        if r + step < window:
            below = read(p + 1, r + 1)
        else:
            below = jnp.where(line == step - 1, 0.0, pltpu.roll(core, step - 1, 0))
        left = jnp.where(lane == 0, 0.0, pltpu.roll(core, 1, 1))
        right = jnp.where(lane == cols - 1, 0.0, pltpu.roll(core, cols - 1, 1))
        return core, read(p, r) + read(p + 2, r) + above + below + left + right

    def reader(key):
        return lambda p, r: field[slots[key], p, pl.ds(r, step)]

    def difference(new, old):
        return lambda p, r: field[slots[new], p, pl.ds(r, step)] - field[slots[old], p, pl.ds(r, step)]

    def piece(ref, p, r):
        return ref[p, pl.ds(r, step)]

    def result(n, end):
        def remote(target, source_slice):
            return pltpu.make_async_remote_copy(
                src_ref=field.at[slots[end], inner, pl.ds(own_at, own_rows)],
                dst_ref=out_hbm.at[0, :, pl.ds(pl.multiple_of(source_slice * own_rows, 8), own_rows)],
                send_sem=out_send.at[target],
                recv_sem=out_recv.at[source_slice],
                device_id={"tm": target},
            )
        return remote

    def own_copy(n):
        return pltpu.make_async_copy(
            field.at[slots[ends[n]], inner, pl.ds(own_at, own_rows)],
            out_hbm.at[0, :, pl.ds(n * own_rows, own_rows)],
            own_sem.at[1],
        )

    def emit(key):
        for n, end in enumerate(ends):
            if end == key:

                @pl.when(t != n)
                def _():
                    result(n, end)(n, t).start()

                @pl.when(t == n)
                def _():
                    own_copy(n).start()

    for tasks in rounds:
        for task in tasks:
            if task[0] == "coarse":
                _, n, source_key, target = task
                arrive(source_key)
                for i, p, r in pieces:
                    core, around = neighbours(reader(source_key), p, r)
                    field[slots[target], p + 1, pl.ds(r, step)] = core + piece(scale, p, r) * (
                        around - 6.0 * core + piece(forcing.at[n], p, r)
                    )
                    if i == 0 and r + step == window:
                        send(target, (0,))
            else:
                _, n, source_key, target, j, pair = task
                held = source_key[0] % 2 * slices + n
                arrive(source_key)
                if pair is not None:
                    arrive(pair[0])
                    arrive(pair[1])
                for i, p, r in pieces:
                    core, around = neighbours(reader(source_key), p, r)
                    gain = piece(inv, p, r)
                    if j == 1:
                        constant = core - gain * (6.0 * step_fine * core - step_fine * piece(forcing.at[n], p, r))
                        base[held, p, pl.ds(r, step)] = constant
                    else:
                        constant = piece(base.at[held], p, r)
                    value = constant + step_fine * gain * around
                    if pair is not None:
                        change, spread = neighbours(difference(*pair), p, r)
                        value = value + change + piece(scale, p, r) * (spread - 6.0 * change)
                    field[slots[target], p + 1, pl.ds(r, step)] = value
                    if i == 0 and r + step == window:
                        send(target, (0,))
            send(target, (1,))
            emit(target)

    for key in sorted(sent):
        arrive(key)
        for side, there in ((0, low_there), (1, high_there)):

            @pl.when(there)
            def _():
                halo(key, side).wait_send()

    for copy in ctrl_copies:
        copy.wait_send()
    for n in range(slices):

        @pl.when(t != n)
        def _():
            result(n, ends[n])(n, t).wait_send()
            result(n, ends[n])(t, n).wait_recv()

        @pl.when(t == n)
        def _():
            own_copy(n).wait()


def wide_kernel(size, state_hbm, cap_hbm, src_hbm, ctrl_ref, seg_ref, out_hbm,
                stage, given, inv, scale, bounds, coarse, sweep, base, near, change, state, end,
                seg_all, ctrl_all, load_sem, own_sem, in_send, in_recv, seg_send, seg_recv,
                ctrl_send, ctrl_recv, side_send, side_recv, mid_send, mid_recv,
                out_send, out_recv, last_sem, level_sem, ring_sem):
    planes, rows, cols, slices, count, own = size
    total = planes * count
    devices = slices * count
    window, pad, lanes = 3 * own, 8, 128
    parts = cols // lanes
    mine = pl.ds(pad + own, own)
    whole = pl.ds(1, total)
    t = lax.axis_index("tm")
    s = lax.axis_index("space")

    def swap(x):
        return x + x % 4 // 2 * (1 - 2 * (x % 2))

    def turn(x, level):
        return x + level % 2 * (slices - 1 - 2 * x)

    def index(t, s):
        chip = s // 2 * slices + turn(swap(t), s // 2)
        return 2 * chip + (s + chip) % 2

    def place(i):
        chip = i // 2
        level = chip // slices
        return swap(turn(chip % slices, level)), 2 * level + (i + chip) % 2

    here = index(t, s)
    has_low, has_high = here > 0, here < devices - 1

    def block(i):
        return pl.ds(pl.multiple_of(i * own, own), own)

    inputs = (state_hbm, cap_hbm, src_hbm)
    order = (1, 0, 2)
    loads = [
        [
            pltpu.make_async_copy(
                inputs[a].at[:, :, pl.ds(h * lanes, lanes)], stage.at[a, :, h], load_sem.at[a, h]
            )
            for h in range(parts)
        ]
        for a in range(3)
    ]
    owns = [
        [
            pltpu.make_async_copy(
                inputs[a].at[:, block(here), pl.ds(h * lanes, lanes)],
                given.at[a, pl.ds(1 + planes * s, planes), h, mine],
                own_sem.at[a, h],
            )
            for h in range(parts)
        ]
        for a in range(3)
    ]
    for group in (loads, owns):
        for a in order:
            for copy in group[a]:
                copy.start()
    own_seg = pltpu.make_async_copy(seg_ref, seg_all.at[s], last_sem.at[1])
    own_ctrl = pltpu.make_async_copy(ctrl_ref, ctrl_all.at[0], last_sem.at[2])

    seg_all[...] = jnp.zeros(seg_all.shape, jnp.int32)
    levels = count // 2
    level, core = s // 2, s % 2
    spot = swap(t)
    ring_ids = [{"tm": swap(lax.rem(spot + hop, slices))} for hop in (1, slices - 1)]
    has_down, has_up = level > 0, level < levels - 1
    beside = jnp.minimum(level, 1) + jnp.minimum(levels - 1 - level, 1)

    def signal_levels(semaphore):
        for there, shift in ((has_down, -1), (has_up, 1)):

            @pl.when(there)
            def _():
                for other in (0, 1):
                    pl.semaphore_signal(semaphore, inc=1, device_id={"space": 2 * (level + shift) + other})

    barrier = pltpu.get_barrier_semaphore()
    signal_levels(barrier)
    pl.semaphore_signal(barrier, inc=1, device_id={"space": s + 1 - 2 * core})
    for ring_id in ring_ids:
        pl.semaphore_signal(barrier, inc=1, device_id=ring_id)

    flat = jnp.zeros((parts, window + 2 * pad, lanes), jnp.float32)
    for plane in (0, total + 1):
        given[0, plane] = flat
        for ref in (coarse, sweep, change, state):
            for k in range(ref.shape[0]):
                ref[k, plane] = flat
    for missing, at in ((has_low, pad), (has_high, pad + 2 * own)):

        @pl.when(jnp.logical_not(missing))
        def _():
            side = jnp.zeros((total, parts, own, lanes), jnp.float32)
            given[0, whole, :, pl.ds(at, own)] = side
            given[1, whole, :, pl.ds(at, own)] = side + 1.0
            given[2, whole, :, pl.ds(at, own)] = side
            for k in range(state.shape[0]):
                state[k, whole, :, pl.ds(at, own)] = side

    pl.semaphore_wait(barrier, 3 + 2 * beside)

    def spread(a, target, source):
        return pltpu.make_async_remote_copy(
            src_ref=stage.at[a, :, :, block(index(t, target))],
            dst_ref=given.at[a, pl.ds(1 + planes * source, planes), :, mine],
            send_sem=in_send.at[a, target],
            recv_sem=in_recv.at[a, source],
            device_id={"space": target},
        )

    def spread_seg(target, source):
        return pltpu.make_async_remote_copy(
            src_ref=seg_ref,
            dst_ref=seg_all.at[source],
            send_sem=seg_send.at[target],
            recv_sem=seg_recv.at[source],
            device_id={"space": target},
        )

    def side(origin, target, send_sem, recv_sem, upward):
        other_t, other_s = place(here + 1 if upward else here - 1)
        return pltpu.make_async_remote_copy(
            src_ref=origin.at[whole, :, mine],
            dst_ref=target.at[whole, :, pl.ds(pad if upward else pad + 2 * own, own)],
            send_sem=send_sem.at[int(upward)],
            recv_sem=recv_sem.at[int(upward)],
            device_id={"tm": other_t, "space": other_s},
        )

    def side_start(*args):
        for upward, there in ((False, has_low), (True, has_high)):

            @pl.when(there)
            def _():
                side(*args, upward).start()

    def side_recv_wait(*args):
        for upward, there in ((True, has_low), (False, has_high)):

            @pl.when(there)
            def _():
                side(*args, upward).wait_recv()

    def side_send_wait(*args):
        for upward, there in ((False, has_low), (True, has_high)):

            @pl.when(there)
            def _():
                side(*args, upward).wait_send()

    def given_side(a):
        return given.at[a], given.at[a], side_send.at[a], side_recv.at[a]

    def state_side(n):
        return near.at[n - 1], state.at[n - 1], mid_send.at[n - 1], mid_recv.at[n - 1]

    def spread_far(a, distance):
        for shift in (-distance, distance):
            there = jnp.logical_and(level + shift >= 0, level + shift < levels)

            @pl.when(there)
            def _():
                for other in (0, 1):
                    spread(a, 2 * (level + shift) + other, s).start()

    def spread_near(a):
        for copy in loads[a]:
            copy.wait()
        spread_far(a, 1)
        spread(a, s + 1 - 2 * core, s).start()

    def pass_ctrl(step):
        return pltpu.make_async_remote_copy(
            src_ref=ctrl_all.at[step - 1] if step > 1 else ctrl_ref,
            dst_ref=ctrl_all.at[step],
            send_sem=ctrl_send.at[step],
            recv_sem=ctrl_recv.at[step],
            device_id=ring_ids[0],
        )

    spread_near(order[0])
    if levels > 2:
        signal_levels(level_sem.at[0])
    spread_near(order[1])
    for distance in range(2, levels):
        pl.semaphore_wait(level_sem.at[distance - 2], 2 * beside)
        if distance + 1 < levels:
            signal_levels(level_sem.at[distance - 1])
        spread_far(order[0], distance)
    for distance in range(2, levels):
        spread_far(order[1], distance)
    spread_near(order[2])
    for distance in range(2, levels):
        spread_far(order[2], distance)
    own_seg.start()
    own_ctrl.start()
    pass_ctrl(1).start()

    step = 2
    row_id = lax.broadcasted_iota(jnp.int32, (step, parts, window, lanes), 2) + (here - 1) * own
    inside = jnp.logical_and(row_id >= 0, row_id < rows)
    all_rows = pl.ds(pad, window)

    def collect(a):
        for copy in owns[a]:
            copy.wait()
        for hop in range(1, count):
            source = lax.rem(s + count - hop, count)
            spread(a, s, source).wait_recv()
        side_start(*given_side(a))

    collect(1)
    for ring_id in ring_ids:
        pl.semaphore_signal(ring_sem.at[0], inc=1, device_id=ring_id)
    for target in (0, 1):

        @pl.when(jnp.logical_and(t == 0, s != target))
        def _():
            spread_seg(target, s).start()

    for hop in range(1, slices - 1):
        pass_ctrl(hop).wait_recv()
        pass_ctrl(hop + 1).start()
    collect(0)
    side_recv_wait(*given_side(1))
    for p in range(0, total, step):
        capacity = given[1, pl.ds(p + 1, step), :, all_rows]
        scale[pl.ds(p, step), :, all_rows] = jnp.where(inside, step_coarse / capacity, 0.0)
        inv[pl.ds(p, step), :, all_rows] = jnp.where(inside, 1.0 / (capacity + 6.0 * step_fine), 0.0)

    own_seg.wait()
    own_ctrl.wait()
    pass_ctrl(slices - 1).wait_recv()
    for target in (0, 1):

        @pl.when(jnp.logical_and(t == 0, s == target))
        def _():
            for hop in range(1, count):
                source = (target + hop) % count
                spread_seg(target, source).wait_recv()

    segments = ctrl_ref.shape[1]
    for n in range(slices):
        row = jnp.zeros((1, segments), jnp.float32)
        for hop in range(slices):
            row = jnp.where(lax.rem(spot - swap(n) + slices, slices) == hop, ctrl_all[hop], row)
        for source in range(count):
            segment = seg_all[source]
            values = jnp.zeros((planes, cols), jnp.float32)
            for k in range(segments):
                values = jnp.where(segment == k, row[:, k:k + 1], values)
            for plane in range(planes):
                for h in range(parts):
                    bounds[n, source * planes + plane, h] = jnp.broadcast_to(
                        values[plane:plane + 1, h * lanes:(h + 1) * lanes], (8, lanes)
                    )

    collect(2)
    side_recv_wait(*given_side(0))
    side_recv_wait(*given_side(2))

    lane = lax.broadcasted_iota(jnp.int32, (step, 8, lanes), 2)
    lane_low, lane_high = lane == 0, lane == lanes - 1

    def extent(reach):
        extra = -(-reach // 4) * 4
        return own - extra, own + 2 * extra

    def load(ref, p, h, at, height):
        return ref[pl.ds(p, step), h, pl.ds(pad + at, height)]

    def rotate(value, amount):
        return pltpu.roll(value, amount % lanes, 2)

    def around(ref, p, at, height):
        cores, sums = [], []
        for h in range(parts):
            block = ref[pl.ds(p, step + 2), h, pl.ds(pad + at, height)]
            cores.append(block[1:step + 1])
            sums.append(block[:step] + block[2:] + (
                load(ref, p + 1, h, at - 1, height) + load(ref, p + 1, h, at + 1, height)
            ))
        ups = [rotate(core, 1) for core in cores]
        downs = [rotate(core, -1) for core in cores]
        low = jnp.concatenate([lane_low] * (height // 8), axis=1)
        high = jnp.concatenate([lane_high] * (height // 8), axis=1)
        for h in range(parts):
            left = jnp.where(low, ups[h - 1] if h else 0.0, ups[h])
            right = jnp.where(high, downs[h + 1] if h + 1 < parts else 0.0, downs[h])
            sums[h] = sums[h] + (left + right)
        return cores, sums

    def row_mask(at, height):
        row_id = lax.broadcasted_iota(jnp.int32, (step, height, lanes), 1) + ((here - 1) * own + at)
        return row_id == 0

    def begin(start, n, target, hold, ahead, reach):
        at, height = extent(reach)
        first_row = row_mask(at, height)
        for p in range(0, total, step):
            cores, sums = around(start, p, at, height)
            for h in range(parts):
                edge = jnp.concatenate([bounds[n, pl.ds(p, step), h]] * (height // 8), axis=1)
                gain = load(inv, p, h, at, height)
                drive = load(given.at[2], p + 1, h, at, height) + jnp.where(first_row, edge, 0.0)
                drive = drive - 6.0 * step_fine * cores[h]
                constant = cores[h] + gain * drive
                hold[pl.ds(p, step), h, pl.ds(pad + at, height)] = constant
                target[pl.ds(p + 1, step), h, pl.ds(pad + at, height)] = constant + gain * sums[h]
                if ahead is not None:
                    ahead[pl.ds(p + 1, step), h, pl.ds(pad + at, height)] = cores[h] + load(
                        scale, p, h, at, height
                    ) * (drive + sums[h])

    def go_on(source, hold, target, reach):
        at, height = extent(reach)
        for p in range(0, total, step):
            _, sums = around(source, p, at, height)
            for h in range(parts):
                target[pl.ds(p + 1, step), h, pl.ds(pad + at, height)] = load(
                    hold, p, h, at, height
                ) + load(inv, p, h, at, height) * sums[h]

    def finish(source, hold, pair, target, reach):
        if pair is not None:
            new, old, moved = pair
            at, height = extent(reach + 1)
            for p in range(0, total, step):
                for h in range(parts):
                    moved[pl.ds(p + 1, step), h, pl.ds(pad + at, height)] = load(
                        new, p + 1, h, at, height
                    ) - load(old, p + 1, h, at, height)
        at, height = extent(reach)
        for p in range(0, total, step):
            _, sums = around(source, p, at, height)
            if pair is not None:
                cores, spreads = around(moved, p, at, height)
            for h in range(parts):
                value = load(hold, p, h, at, height) + load(inv, p, h, at, height) * sums[h]
                if pair is not None:
                    value = value + (cores[h] + load(scale, p, h, at, height) * (spreads[h] - 6.0 * cores[h]))
                target[pl.ds(p + 1, step), h, pl.ds(pad + at, height)] = value

    def solve(number, start, n, ahead, pair, target, reach):
        a, b, hold = sweep.at[2 * number], sweep.at[2 * number + 1], base.at[number]
        begin(start, n, a, hold, ahead, reach + SWEEPS - 1)
        for j in range(2, SWEEPS):
            go_on(a, hold, b, reach + SWEEPS - j)
            a, b = b, a
        finish(a, hold, pair, target, reach)

    def deliver(n, target_s, source_t, source_s, ref):
        return pltpu.make_async_remote_copy(
            src_ref=ref.at[pl.ds(1 + planes * target_s, planes), :, mine],
            dst_ref=out_hbm.at[:, index(source_t, source_s)],
            send_sem=out_send.at[n, target_s],
            recv_sem=out_recv.at[source_t, source_s],
            device_id={"tm": n, "space": target_s},
        )

    def keep_local(n):
        return pltpu.make_async_copy(
            result[n].at[pl.ds(1 + planes * s, planes), :, mine], out_hbm.at[:, here], last_sem.at[0]
        )

    result = [near.at[0]] + [end.at[n - 1] for n in range(1, slices)]

    def emit(n):
        for hop in range(1, count):
            deliver(n, lax.rem(s + hop, count), t, s, result[n]).start()

        @pl.when(t != n)
        def _():
            deliver(n, s, t, s, result[n]).start()

        @pl.when(t == n)
        def _():
            keep_local(n).start()

    starts = [given.at[0]] + [coarse.at[n - 1] for n in range(1, slices - 1)]
    for n in range(slices - 1):
        ahead = coarse.at[n] if n + 2 < slices else None
        pair = (near.at[n - 1], starts[n], change.at[n - 1]) if n else None
        solve(n, starts[n], n, ahead, pair, near.at[n], slices - 2 - n)
        side_start(*state_side(n + 1))
        for p in range(0, total, step):
            state[n, pl.ds(p + 1, step), :, mine] = near[n, pl.ds(p + 1, step), :, mine]
    for far in range(1, slices // 2):
        pl.semaphore_wait(ring_sem.at[far - 1], 2)
        for ring_id in ring_ids:
            pl.semaphore_signal(ring_sem.at[far], inc=1, device_id=ring_id)
    pl.semaphore_wait(ring_sem.at[slices // 2 - 1], 2)
    emit(0)
    for n in range(1, slices):
        side_recv_wait(*state_side(n))
        pair = (end.at[n - 2], state.at[n - 1], change.at[slices + n - 4]) if n > 1 else None
        solve(slices - 2 + n, state.at[n - 1], n, None, pair, end.at[n - 1], slices - 1 - n)
        emit(n)

    for a in range(3):
        for hop in range(1, count):
            spread(a, lax.rem(s + hop, count), s).wait_send()
        side_send_wait(*given_side(a))
    for hop in range(1, slices):
        pass_ctrl(hop).wait_send()
    for target in (0, 1):

        @pl.when(jnp.logical_and(t == 0, s != target))
        def _():
            spread_seg(target, s).wait_send()

    for n in range(1, slices):
        side_send_wait(*state_side(n))
    for n in range(slices):
        for hop in range(1, count):
            deliver(n, lax.rem(s + hop, count), t, s, result[n]).wait_send()

        @pl.when(t != n)
        def _():
            deliver(n, s, t, s, result[n]).wait_send()

        @pl.when(t == n)
        def _():
            keep_local(n).wait()

    for hop_t in range(slices):
        for hop_s in range(count):
            if hop_t or hop_s:
                source_t, source_s = lax.rem(t + hop_t, slices), lax.rem(s + hop_s, count)
                deliver(t, s, source_t, source_s, result[0]).wait_recv()


def wide_fits(slices, count, rows, cols):
    own = rows // (slices * count)
    ordered = slices % 4 in (0, 2) and slices < 8 and count % 2 == 0
    return ordered and CORRECTIONS == 2 and slices > 2 and own == 8 and own >= SWEEPS + slices - 2 \
        and rows == own * slices * count and cols % 128 == 0


def solution(mesh):
    slices, count = mesh.shape["tm"], mesh.shape["space"]
    plan = make_plan(slices)

    def wide(initial_state, capacity, source, control, segment_index):
        planes, rows, cols = initial_state.shape
        own = rows // (slices * count)
        total, window, parts = planes * count, 3 * own, cols // 128
        still = (total, parts, window + 16, 128)
        size = (planes, rows, cols, slices, count, own)
        dma = pltpu.SemaphoreType.DMA

        def fields(number):
            return pltpu.VMEM((number, total + 2, parts, window + 16, 128), jnp.float32)

        result = pl.pallas_call(
            functools.partial(wide_kernel, size),
            out_shape=jax.ShapeDtypeStruct((planes, rows // own, parts, own, 128), jnp.float32),
            in_specs=[pl.BlockSpec(memory_space=pl.ANY)] * 3 + [pl.BlockSpec(memory_space=pltpu.VMEM)] * 2,
            out_specs=pl.BlockSpec(memory_space=pl.ANY),
            scratch_shapes=[
                pltpu.VMEM((3, planes, parts, rows, 128), jnp.float32),
                fields(3),
                pltpu.VMEM(still, jnp.float32),
                pltpu.VMEM(still, jnp.float32),
                pltpu.VMEM((slices, total, parts, 8, 128), jnp.float32),
                fields(slices - 2),
                fields(4 * (slices - 1)),
                pltpu.VMEM((2 * (slices - 1),) + still, jnp.float32),
                fields(slices - 1),
                fields(2 * (slices - 2)),
                fields(slices - 1),
                fields(slices - 1),
                pltpu.VMEM((count,) + segment_index.shape, jnp.int32),
                pltpu.VMEM((slices,) + control.shape, jnp.float32),
                dma((3, parts)),
                dma((3, parts)),
                dma((3, count)),
                dma((3, count)),
                dma((count,)),
                dma((count,)),
                dma((slices,)),
                dma((slices,)),
                dma((3, 2)),
                dma((3, 2)),
                dma((slices - 1, 2)),
                dma((slices - 1, 2)),
                dma((slices, count)),
                dma((slices, count)),
                dma((3,)),
                pltpu.SemaphoreType.REGULAR((max(count // 2 - 2, 1),)),
                pltpu.SemaphoreType.REGULAR((slices // 2,)),
            ],
            compiler_params=pltpu.CompilerParams(
                collective_id=0, has_side_effects=True, vmem_limit_bytes=67043328 - 1048576
            ),
        )(initial_state, capacity, source, control, segment_index)
        return result.transpose(0, 1, 3, 2, 4).reshape(1, planes, rows, cols)

    def on_device(initial_state, capacity, source, control, segment_index):
        planes, rows, cols = initial_state.shape
        if wide_fits(slices, count, rows, cols):
            return wide(initial_state, capacity, source, control, segment_index)
        own_rows = rows // slices
        reach = -(-(CORRECTIONS * SWEEPS + slices - CORRECTIONS) // 8) * 8
        window = min(rows, own_rows + 2 * reach)
        fields = len(plan[0])
        size = (planes, window, own_rows, reach, rows, cols, slices, count)
        block = (planes, window, cols)
        dma = pltpu.SemaphoreType.DMA
        return pl.pallas_call(
            functools.partial(kernel, plan, size),
            out_shape=jax.ShapeDtypeStruct((1, planes, rows, cols), jnp.float32),
            in_specs=[pl.BlockSpec(memory_space=pl.ANY)] * 3 + [pl.BlockSpec(memory_space=pltpu.VMEM)] * 2,
            out_specs=pl.BlockSpec(memory_space=pl.ANY),
            scratch_shapes=[
                pltpu.VMEM((fields, planes + 2, window, cols), jnp.float32),
                pltpu.VMEM((slices,) + block, jnp.float32),
                pltpu.VMEM((2 * slices,) + block, jnp.float32),
                pltpu.VMEM(block, jnp.float32),
                pltpu.VMEM(block, jnp.float32),
                pltpu.VMEM(block, jnp.float32),
                pltpu.VMEM((slices,) + control.shape, jnp.float32),
                dma((fields, 2)),
                dma((fields, 2)),
                dma((3,)),
                dma((slices,)),
                dma((slices,)),
                dma((slices,)),
                dma((slices,)),
                dma((2,)),
            ],
            compiler_params=pltpu.CompilerParams(
                collective_id=0, has_side_effects=True, vmem_limit_bytes=67043328 - 1048576
            ),
        )(initial_state, capacity, source, control, segment_index)

    return jax.shard_map(
        on_device,
        mesh=mesh,
        in_specs=(
            P("space", None, None),
            P("space", None, None),
            P("space", None, None),
            P("tm", None),
            P("space", None),
        ),
        out_specs=P("tm", "space", None, None),
        check_vma=False,
    )
```

```python
import functools

import jax
import jax.numpy as jnp
from jax import lax
from jax.experimental import pallas as pl
from jax.experimental.pallas import tpu as pltpu
from jax.sharding import PartitionSpec as P

SWEEPS = 6
CORRECTIONS = 2
step_fine = 1.0
step_coarse = 0.08


def make_plan(slices):
    last = CORRECTIONS
    solves = [
        (k, n)
        for k in range(last)
        for n in range(k, slices)
        if k == last - 1 or n + 1 < slices or n == k
    ]
    slots, sent = {}, set()
    for k, n in solves:
        for j in range(SWEEPS):
            slots[(k, n, j)] = len(slots)
            sent.add((k, n, j))

    def state(k, n):
        k = min(k, n)
        key = (k, n, 0)
        if key not in slots:
            slots[key] = len(slots)
        return key

    ends = [state(last, n + 1) for n in range(slices)]
    rounds = {}
    top_coarse = max(n for k, n in solves if k == 0)
    for n in range(top_coarse):
        rounds.setdefault(n + 1, []).append(("coarse", n, state(0, n), state(0, n + 1)))
    for k, n in sorted(solves, key=lambda item: (-item[0], item[1])):
        begin = SWEEPS * k + n - k
        for j in range(1, SWEEPS + 1):
            target = (k, n, j) if j < SWEEPS else state(k + 1, n + 1)
            pair = None
            if j == SWEEPS and k < n:
                pair = (state(k + 1, n), state(k, n))
                sent.add(pair[0])
                sent.add(pair[1])
            rounds.setdefault(begin + j, []).append(("sweep", n, (k, n, j - 1), target, j, pair))
    return slots, sent, [rounds[r] for r in sorted(rounds)], ends


def kernel(plan, size, state_hbm, cap_hbm, src_hbm, ctrl_ref, seg_ref, out_hbm,
           field, forcing, base, inv, scale, source, ctrl_all,
           send_sem, recv_sem, in_sem, ctrl_send, ctrl_recv, out_send, out_recv, own_sem):
    slots, sent, rounds, ends = plan
    planes, window, own_rows, reach, rows, cols, slices, count = size
    t = lax.axis_index("tm")
    s = lax.axis_index("space")
    low_there, high_there = s > 0, s < count - 1
    first_row = pl.multiple_of(jnp.clip(t * own_rows - reach, 0, rows - window), 8)
    own_at = pl.multiple_of(t * own_rows - first_row, 8)
    inner = pl.ds(1, planes)
    first = slots[(0, 0, 0)]

    loads = []
    for index, (ref, target) in enumerate(
        ((state_hbm, field.at[first, inner]), (cap_hbm, inv), (src_hbm, source))
    ):
        loads.append(pltpu.make_async_copy(ref.at[:, pl.ds(first_row, window), :], target, in_sem.at[index]))
        loads[-1].start()

    @pl.when(jnp.logical_not(low_there))
    def _():
        for key in sorted(sent):
            field[slots[key], 0] = jnp.zeros((window, cols), jnp.float32)

    @pl.when(jnp.logical_not(high_there))
    def _():
        for key in sorted(sent):
            field[slots[key], planes + 1] = jnp.zeros((window, cols), jnp.float32)

    barrier = pltpu.get_barrier_semaphore()

    @pl.when(low_there)
    def _():
        pl.semaphore_signal(barrier, inc=1, device_id={"space": s - 1})

    @pl.when(high_there)
    def _():
        pl.semaphore_signal(barrier, inc=1, device_id={"space": s + 1})

    for hop in range(1, slices):
        pl.semaphore_signal(barrier, inc=1, device_id={"tm": lax.rem(t + hop, slices)})
    pl.semaphore_wait(barrier, slices - 1 + jnp.minimum(s, 1) + jnp.minimum(count - 1 - s, 1))

    def halo(key, side):
        slot = slots[key]
        if side == 0:
            source_plane, target_plane, other = 1, planes + 1, s - 1
        else:
            source_plane, target_plane, other = planes, 0, s + 1
        k, n, j = key
        left = CORRECTIONS * (SWEEPS - 1) + slices - (k * (SWEEPS - 1) + n + j)
        near = min(-(-left // 8) * 8, reach)
        height = min(window, own_rows + 2 * near)
        at = jnp.clip(t * own_rows - near, 0, rows - height) - first_row
        needed = pl.ds(pl.multiple_of(at, 8), height)
        return pltpu.make_async_remote_copy(
            src_ref=field.at[slot, source_plane, needed],
            dst_ref=field.at[slot, target_plane, needed],
            send_sem=send_sem.at[slot, side],
            recv_sem=recv_sem.at[slot, side],
            device_id={"space": other},
        )

    odd = lax.rem(s, 2)

    def send(key, parts=(0, 1)):
        if key in sent:
            for part in parts:
                for side, there in ((0, low_there), (1, high_there)):

                    @pl.when(jnp.logical_and(there, odd == (side + part) % 2))
                    def _():
                        halo(key, side).start()

    arrived = set()

    def arrive(key):
        if key in arrived:
            return
        arrived.add(key)
        for side, there in ((0, high_there), (1, low_there)):

            @pl.when(there)
            def _():
                halo(key, side).wait_recv()

    loads[0].wait()
    send((0, 0, 0))

    ctrl_copies = []
    for hop in range(1, slices):
        ctrl_copies.append(pltpu.make_async_remote_copy(
            src_ref=ctrl_ref,
            dst_ref=ctrl_all.at[hop],
            send_sem=ctrl_send.at[hop],
            recv_sem=ctrl_recv.at[hop],
            device_id={"tm": lax.rem(t + hop, slices)},
        ))
        ctrl_copies[-1].start()
    own_ctrl = pltpu.make_async_copy(ctrl_ref, ctrl_all.at[0], own_sem.at[0])
    own_ctrl.start()

    loads[1].wait()
    capacity = inv[...]
    scale[...] = step_coarse / capacity
    reciprocal = 1.0 / (capacity + 6.0 * step_fine)
    inv[...] = reciprocal
    loads[2].wait()
    own_ctrl.wait()
    for copy in ctrl_copies:
        copy.wait_recv()

    segment = seg_ref[...]
    segments = ctrl_ref.shape[1]
    row_id = lax.broadcasted_iota(jnp.int32, (planes, window, cols), 1) + first_row
    for n in range(slices):
        row = jnp.zeros((1, segments), jnp.float32)
        for hop in range(slices):
            row = jnp.where(lax.rem(t - n + slices, slices) == hop, ctrl_all[hop], row)
        values = jnp.zeros((planes, cols), jnp.float32)
        for k in range(segments):
            values = jnp.where(segment == k, row[:, k:k + 1], values)
        forcing[n] = source[...] + jnp.where(row_id == 0, values[:, None, :], 0.0)

    step = window // 2 if window % 16 == 0 else window
    lane = lax.broadcasted_iota(jnp.int32, (step, cols), 1)
    line = lax.broadcasted_iota(jnp.int32, (step, cols), 0)
    pieces = []
    for i in range(planes):
        p = jnp.where(odd == 1, planes - 1 - i, i)
        pieces += [(i, p, r) for r in range(0, window, step)]

    def neighbours(read, p, r):
        core = read(p + 1, r)
        if r > 0:
            above = read(p + 1, r - 1)
        else:
            above = jnp.where(line == 0, 0.0, pltpu.roll(core, 1, 0))
        if r + step < window:
            below = read(p + 1, r + 1)
        else:
            below = jnp.where(line == step - 1, 0.0, pltpu.roll(core, step - 1, 0))
        left = jnp.where(lane == 0, 0.0, pltpu.roll(core, 1, 1))
        right = jnp.where(lane == cols - 1, 0.0, pltpu.roll(core, cols - 1, 1))
        return core, read(p, r) + read(p + 2, r) + above + below + left + right

    def reader(key):
        return lambda p, r: field[slots[key], p, pl.ds(r, step)]

    def difference(new, old):
        return lambda p, r: field[slots[new], p, pl.ds(r, step)] - field[slots[old], p, pl.ds(r, step)]

    def piece(ref, p, r):
        return ref[p, pl.ds(r, step)]

    def result(n, end):
        def remote(target, source_slice):
            return pltpu.make_async_remote_copy(
                src_ref=field.at[slots[end], inner, pl.ds(own_at, own_rows)],
                dst_ref=out_hbm.at[0, :, pl.ds(pl.multiple_of(source_slice * own_rows, 8), own_rows)],
                send_sem=out_send.at[target],
                recv_sem=out_recv.at[source_slice],
                device_id={"tm": target},
            )
        return remote

    def own_copy(n):
        return pltpu.make_async_copy(
            field.at[slots[ends[n]], inner, pl.ds(own_at, own_rows)],
            out_hbm.at[0, :, pl.ds(n * own_rows, own_rows)],
            own_sem.at[1],
        )

    def emit(key):
        for n, end in enumerate(ends):
            if end == key:

                @pl.when(t != n)
                def _():
                    result(n, end)(n, t).start()

                @pl.when(t == n)
                def _():
                    own_copy(n).start()

    for tasks in rounds:
        for task in tasks:
            if task[0] == "coarse":
                _, n, source_key, target = task
                arrive(source_key)
                for i, p, r in pieces:
                    core, around = neighbours(reader(source_key), p, r)
                    field[slots[target], p + 1, pl.ds(r, step)] = core + piece(scale, p, r) * (
                        around - 6.0 * core + piece(forcing.at[n], p, r)
                    )
                    if i == 0 and r + step == window:
                        send(target, (0,))
            else:
                _, n, source_key, target, j, pair = task
                held = source_key[0] % 2 * slices + n
                arrive(source_key)
                if pair is not None:
                    arrive(pair[0])
                    arrive(pair[1])
                for i, p, r in pieces:
                    core, around = neighbours(reader(source_key), p, r)
                    gain = piece(inv, p, r)
                    if j == 1:
                        constant = core - gain * (6.0 * step_fine * core - step_fine * piece(forcing.at[n], p, r))
                        base[held, p, pl.ds(r, step)] = constant
                    else:
                        constant = piece(base.at[held], p, r)
                    value = constant + step_fine * gain * around
                    if pair is not None:
                        change, spread = neighbours(difference(*pair), p, r)
                        value = value + change + piece(scale, p, r) * (spread - 6.0 * change)
                    field[slots[target], p + 1, pl.ds(r, step)] = value
                    if i == 0 and r + step == window:
                        send(target, (0,))
            send(target, (1,))
            emit(target)

    for key in sorted(sent):
        arrive(key)
        for side, there in ((0, low_there), (1, high_there)):

            @pl.when(there)
            def _():
                halo(key, side).wait_send()

    for copy in ctrl_copies:
        copy.wait_send()
    for n in range(slices):

        @pl.when(t != n)
        def _():
            result(n, ends[n])(n, t).wait_send()
            result(n, ends[n])(t, n).wait_recv()

        @pl.when(t == n)
        def _():
            own_copy(n).wait()


def wide_kernel(size, state_hbm, cap_hbm, src_hbm, ctrl_ref, seg_ref, out_hbm,
                stage, given, inv, scale, bounds, coarse, sweep, base, near, change, state, end,
                seg_all, ctrl_all, load_sem, own_sem, in_send, in_recv, seg_send, seg_recv,
                ctrl_send, ctrl_recv, side_send, side_recv, mid_send, mid_recv,
                out_send, out_recv, last_sem, level_sem, ring_sem):
    planes, rows, cols, slices, count, own = size
    total = planes * count
    devices = slices * count
    window, pad, lanes = 3 * own, 8, 128
    parts = cols // lanes
    mine = pl.ds(pad + own, own)
    whole = pl.ds(1, total)
    t = lax.axis_index("tm")
    s = lax.axis_index("space")

    def swap(x):
        return x + x % 4 // 2 * (1 - 2 * (x % 2))

    def turn(x, level):
        return x + level % 2 * (slices - 1 - 2 * x)

    def index(t, s):
        chip = s // 2 * slices + turn(swap(t), s // 2)
        return 2 * chip + (s + chip) % 2

    def place(i):
        chip = i // 2
        level = chip // slices
        return swap(turn(chip % slices, level)), 2 * level + (i + chip) % 2

    here = index(t, s)
    has_low, has_high = here > 0, here < devices - 1

    def block(i):
        return pl.ds(pl.multiple_of(i * own, own), own)

    inputs = (state_hbm, cap_hbm, src_hbm)
    order = (1, 0, 2)
    loads = [
        [
            pltpu.make_async_copy(
                inputs[a].at[:, :, pl.ds(h * lanes, lanes)], stage.at[a, :, h], load_sem.at[a, h]
            )
            for h in range(parts)
        ]
        for a in range(3)
    ]
    owns = [
        [
            pltpu.make_async_copy(
                inputs[a].at[:, block(here), pl.ds(h * lanes, lanes)],
                given.at[a, pl.ds(1 + planes * s, planes), h, mine],
                own_sem.at[a, h],
            )
            for h in range(parts)
        ]
        for a in range(3)
    ]
    for group in (loads, owns):
        for a in order:
            for copy in group[a]:
                copy.start()
    own_seg = pltpu.make_async_copy(seg_ref, seg_all.at[s], last_sem.at[1])
    own_ctrl = pltpu.make_async_copy(ctrl_ref, ctrl_all.at[0], last_sem.at[2])

    seg_all[...] = jnp.zeros(seg_all.shape, jnp.int32)
    levels = count // 2
    level, core = s // 2, s % 2
    spot = swap(t)
    ring_ids = [{"tm": swap(lax.rem(spot + hop, slices))} for hop in (1, slices - 1)]
    has_down, has_up = level > 0, level < levels - 1
    beside = jnp.minimum(level, 1) + jnp.minimum(levels - 1 - level, 1)

    def signal_levels(semaphore):
        for there, shift in ((has_down, -1), (has_up, 1)):

            @pl.when(there)
            def _():
                for other in (0, 1):
                    pl.semaphore_signal(semaphore, inc=1, device_id={"space": 2 * (level + shift) + other})

    barrier = pltpu.get_barrier_semaphore()
    signal_levels(barrier)
    pl.semaphore_signal(barrier, inc=1, device_id={"space": s + 1 - 2 * core})
    for ring_id in ring_ids:
        pl.semaphore_signal(barrier, inc=1, device_id=ring_id)

    flat = jnp.zeros((parts, window + 2 * pad, lanes), jnp.float32)
    for plane in (0, total + 1):
        given[0, plane] = flat
        for ref in (coarse, sweep, change, state):
            for k in range(ref.shape[0]):
                ref[k, plane] = flat
    for missing, at in ((has_low, pad), (has_high, pad + 2 * own)):

        @pl.when(jnp.logical_not(missing))
        def _():
            side = jnp.zeros((total, parts, own, lanes), jnp.float32)
            given[0, whole, :, pl.ds(at, own)] = side
            given[1, whole, :, pl.ds(at, own)] = side + 1.0
            given[2, whole, :, pl.ds(at, own)] = side
            for k in range(state.shape[0]):
                state[k, whole, :, pl.ds(at, own)] = side

    pl.semaphore_wait(barrier, 3 + 2 * beside)

    def spread(a, target, source):
        return pltpu.make_async_remote_copy(
            src_ref=stage.at[a, :, :, block(index(t, target))],
            dst_ref=given.at[a, pl.ds(1 + planes * source, planes), :, mine],
            send_sem=in_send.at[a, target],
            recv_sem=in_recv.at[a, source],
            device_id={"space": target},
        )

    def spread_seg(target, source):
        return pltpu.make_async_remote_copy(
            src_ref=seg_ref,
            dst_ref=seg_all.at[source],
            send_sem=seg_send.at[target],
            recv_sem=seg_recv.at[source],
            device_id={"space": target},
        )

    def side(origin, target, send_sem, recv_sem, upward):
        other_t, other_s = place(here + 1 if upward else here - 1)
        return pltpu.make_async_remote_copy(
            src_ref=origin.at[whole, :, mine],
            dst_ref=target.at[whole, :, pl.ds(pad if upward else pad + 2 * own, own)],
            send_sem=send_sem.at[int(upward)],
            recv_sem=recv_sem.at[int(upward)],
            device_id={"tm": other_t, "space": other_s},
        )

    def side_start(*args):
        for upward, there in ((False, has_low), (True, has_high)):

            @pl.when(there)
            def _():
                side(*args, upward).start()

    def side_recv_wait(*args):
        for upward, there in ((True, has_low), (False, has_high)):

            @pl.when(there)
            def _():
                side(*args, upward).wait_recv()

    def side_send_wait(*args):
        for upward, there in ((False, has_low), (True, has_high)):

            @pl.when(there)
            def _():
                side(*args, upward).wait_send()

    def given_side(a):
        return given.at[a], given.at[a], side_send.at[a], side_recv.at[a]

    def state_side(n):
        return near.at[n - 1], state.at[n - 1], mid_send.at[n - 1], mid_recv.at[n - 1]

    def spread_far(a, distance):
        for shift in (-distance, distance):
            there = jnp.logical_and(level + shift >= 0, level + shift < levels)

            @pl.when(there)
            def _():
                for other in (0, 1):
                    spread(a, 2 * (level + shift) + other, s).start()

    def spread_near(a):
        for copy in loads[a]:
            copy.wait()
        spread_far(a, 1)
        spread(a, s + 1 - 2 * core, s).start()

    def pass_ctrl(step):
        return pltpu.make_async_remote_copy(
            src_ref=ctrl_all.at[step - 1] if step > 1 else ctrl_ref,
            dst_ref=ctrl_all.at[step],
            send_sem=ctrl_send.at[step],
            recv_sem=ctrl_recv.at[step],
            device_id=ring_ids[0],
        )

    own_ctrl.start()
    pass_ctrl(1).start()
    spread_near(order[0])
    if levels > 2:
        signal_levels(level_sem.at[0])
    spread_near(order[1])
    for distance in range(2, levels):
        pl.semaphore_wait(level_sem.at[distance - 2], 2 * beside)
        if distance + 1 < levels:
            signal_levels(level_sem.at[distance - 1])
        spread_far(order[0], distance)
    for distance in range(2, levels):
        spread_far(order[1], distance)
    spread_near(order[2])
    for distance in range(2, levels):
        spread_far(order[2], distance)
    own_seg.start()
    pass_ctrl(1).wait_recv()
    pass_ctrl(2).start()

    step = 2
    row_id = lax.broadcasted_iota(jnp.int32, (step, parts, window, lanes), 2) + (here - 1) * own
    inside = jnp.logical_and(row_id >= 0, row_id < rows)
    all_rows = pl.ds(pad, window)

    def collect(a):
        for copy in owns[a]:
            copy.wait()
        for hop in range(1, count):
            source = lax.rem(s + count - hop, count)
            spread(a, s, source).wait_recv()
        side_start(*given_side(a))

    collect(1)
    for ring_id in ring_ids:
        pl.semaphore_signal(ring_sem.at[0], inc=1, device_id=ring_id)
    for target in (0, 1):

        @pl.when(jnp.logical_and(t == 0, s != target))
        def _():
            spread_seg(target, s).start()

    for hop in range(2, slices - 1):
        pass_ctrl(hop).wait_recv()
        pass_ctrl(hop + 1).start()
    collect(0)
    for far in range(1, slices // 2):
        pl.semaphore_wait(ring_sem.at[far - 1], 2)
        for ring_id in ring_ids:
            pl.semaphore_signal(ring_sem.at[far], inc=1, device_id=ring_id)
    side_recv_wait(*given_side(1))
    for p in range(0, total, step):
        capacity = given[1, pl.ds(p + 1, step), :, all_rows]
        scale[pl.ds(p, step), :, all_rows] = jnp.where(inside, step_coarse / capacity, 0.0)
        inv[pl.ds(p, step), :, all_rows] = jnp.where(inside, 1.0 / (capacity + 6.0 * step_fine), 0.0)

    own_seg.wait()
    own_ctrl.wait()
    pass_ctrl(slices - 1).wait_recv()
    for target in (0, 1):

        @pl.when(jnp.logical_and(t == 0, s == target))
        def _():
            for hop in range(1, count):
                source = (target + hop) % count
                spread_seg(target, source).wait_recv()

    segments = ctrl_ref.shape[1]
    for n in range(slices):
        row = jnp.zeros((1, segments), jnp.float32)
        for hop in range(slices):
            row = jnp.where(lax.rem(spot - swap(n) + slices, slices) == hop, ctrl_all[hop], row)
        for source in range(count):
            segment = seg_all[source]
            values = jnp.zeros((planes, cols), jnp.float32)
            for k in range(segments):
                values = jnp.where(segment == k, row[:, k:k + 1], values)
            for plane in range(planes):
                for h in range(parts):
                    bounds[n, source * planes + plane, h] = jnp.broadcast_to(
                        values[plane:plane + 1, h * lanes:(h + 1) * lanes], (8, lanes)
                    )

    collect(2)
    side_recv_wait(*given_side(0))
    side_recv_wait(*given_side(2))

    lane = lax.broadcasted_iota(jnp.int32, (step, 8, lanes), 2)
    lane_low, lane_high = lane == 0, lane == lanes - 1

    def extent(reach):
        extra = -(-reach // 4) * 4
        return own - extra, own + 2 * extra

    def load(ref, p, h, at, height):
        return ref[pl.ds(p, step), h, pl.ds(pad + at, height)]

    def rotate(value, amount):
        return pltpu.roll(value, amount % lanes, 2)

    def around(ref, p, at, height):
        cores, sums = [], []
        for h in range(parts):
            block = ref[pl.ds(p, step + 2), h, pl.ds(pad + at, height)]
            cores.append(block[1:step + 1])
            sums.append(block[:step] + block[2:] + (
                load(ref, p + 1, h, at - 1, height) + load(ref, p + 1, h, at + 1, height)
            ))
        ups = [rotate(core, 1) for core in cores]
        downs = [rotate(core, -1) for core in cores]
        low = jnp.concatenate([lane_low] * (height // 8), axis=1)
        high = jnp.concatenate([lane_high] * (height // 8), axis=1)
        for h in range(parts):
            left = jnp.where(low, ups[h - 1] if h else 0.0, ups[h])
            right = jnp.where(high, downs[h + 1] if h + 1 < parts else 0.0, downs[h])
            sums[h] = sums[h] + (left + right)
        return cores, sums

    def row_mask(at, height):
        row_id = lax.broadcasted_iota(jnp.int32, (step, height, lanes), 1) + ((here - 1) * own + at)
        return row_id == 0

    def begin(start, n, target, hold, ahead, reach):
        at, height = extent(reach)
        first_row = row_mask(at, height)
        for p in range(0, total, step):
            cores, sums = around(start, p, at, height)
            for h in range(parts):
                edge = jnp.concatenate([bounds[n, pl.ds(p, step), h]] * (height // 8), axis=1)
                gain = load(inv, p, h, at, height)
                drive = load(given.at[2], p + 1, h, at, height) + jnp.where(first_row, edge, 0.0)
                drive = drive - 6.0 * step_fine * cores[h]
                constant = cores[h] + gain * drive
                hold[pl.ds(p, step), h, pl.ds(pad + at, height)] = constant
                target[pl.ds(p + 1, step), h, pl.ds(pad + at, height)] = constant + gain * sums[h]
                if ahead is not None:
                    ahead[pl.ds(p + 1, step), h, pl.ds(pad + at, height)] = cores[h] + load(
                        scale, p, h, at, height
                    ) * (drive + sums[h])

    def go_on(source, hold, target, reach):
        at, height = extent(reach)
        for p in range(0, total, step):
            _, sums = around(source, p, at, height)
            for h in range(parts):
                target[pl.ds(p + 1, step), h, pl.ds(pad + at, height)] = load(
                    hold, p, h, at, height
                ) + load(inv, p, h, at, height) * sums[h]

    def finish(source, hold, pair, target, reach):
        if pair is not None:
            new, old, moved = pair
            at, height = extent(reach + 1)
            for p in range(0, total, step):
                for h in range(parts):
                    moved[pl.ds(p + 1, step), h, pl.ds(pad + at, height)] = load(
                        new, p + 1, h, at, height
                    ) - load(old, p + 1, h, at, height)
        at, height = extent(reach)
        for p in range(0, total, step):
            _, sums = around(source, p, at, height)
            if pair is not None:
                cores, spreads = around(moved, p, at, height)
            for h in range(parts):
                value = load(hold, p, h, at, height) + load(inv, p, h, at, height) * sums[h]
                if pair is not None:
                    value = value + (cores[h] + load(scale, p, h, at, height) * (spreads[h] - 6.0 * cores[h]))
                target[pl.ds(p + 1, step), h, pl.ds(pad + at, height)] = value

    def solve(number, start, n, ahead, pair, target, reach):
        a, b, hold = sweep.at[2 * number], sweep.at[2 * number + 1], base.at[number]
        begin(start, n, a, hold, ahead, reach + SWEEPS - 1)
        for j in range(2, SWEEPS):
            go_on(a, hold, b, reach + SWEEPS - j)
            a, b = b, a
        finish(a, hold, pair, target, reach)

    def deliver(n, target_s, source_t, source_s, ref):
        return pltpu.make_async_remote_copy(
            src_ref=ref.at[pl.ds(1 + planes * target_s, planes), :, mine],
            dst_ref=out_hbm.at[:, index(source_t, source_s)],
            send_sem=out_send.at[n, target_s],
            recv_sem=out_recv.at[source_t, source_s],
            device_id={"tm": n, "space": target_s},
        )

    def keep_local(n):
        return pltpu.make_async_copy(
            result[n].at[pl.ds(1 + planes * s, planes), :, mine], out_hbm.at[:, here], last_sem.at[0]
        )

    result = [near.at[0]] + [end.at[n - 1] for n in range(1, slices)]

    def emit(n):
        for hop in range(1, count):
            deliver(n, lax.rem(s + hop, count), t, s, result[n]).start()

        @pl.when(t != n)
        def _():
            deliver(n, s, t, s, result[n]).start()

        @pl.when(t == n)
        def _():
            keep_local(n).start()

    starts = [given.at[0]] + [coarse.at[n - 1] for n in range(1, slices - 1)]
    for n in range(slices - 1):
        ahead = coarse.at[n] if n + 2 < slices else None
        pair = (near.at[n - 1], starts[n], change.at[n - 1]) if n else None
        solve(n, starts[n], n, ahead, pair, near.at[n], slices - 2 - n)
        side_start(*state_side(n + 1))
        for p in range(0, total, step):
            state[n, pl.ds(p + 1, step), :, mine] = near[n, pl.ds(p + 1, step), :, mine]
    pl.semaphore_wait(ring_sem.at[slices // 2 - 1], 2)
    emit(0)
    for n in range(1, slices):
        side_recv_wait(*state_side(n))
        pair = (end.at[n - 2], state.at[n - 1], change.at[slices + n - 4]) if n > 1 else None
        solve(slices - 2 + n, state.at[n - 1], n, None, pair, end.at[n - 1], slices - 1 - n)
        emit(n)

    for a in range(3):
        for hop in range(1, count):
            spread(a, lax.rem(s + hop, count), s).wait_send()
        side_send_wait(*given_side(a))
    for hop in range(1, slices):
        pass_ctrl(hop).wait_send()
    for target in (0, 1):

        @pl.when(jnp.logical_and(t == 0, s != target))
        def _():
            spread_seg(target, s).wait_send()

    for n in range(1, slices):
        side_send_wait(*state_side(n))
    for n in range(slices):
        for hop in range(1, count):
            deliver(n, lax.rem(s + hop, count), t, s, result[n]).wait_send()

        @pl.when(t != n)
        def _():
            deliver(n, s, t, s, result[n]).wait_send()

        @pl.when(t == n)
        def _():
            keep_local(n).wait()

    for hop_t in range(slices):
        for hop_s in range(count):
            if hop_t or hop_s:
                source_t, source_s = lax.rem(t + hop_t, slices), lax.rem(s + hop_s, count)
                deliver(t, s, source_t, source_s, result[0]).wait_recv()


def wide_fits(slices, count, rows, cols):
    own = rows // (slices * count)
    ordered = slices % 4 in (0, 2) and slices < 8 and count % 2 == 0
    return ordered and CORRECTIONS == 2 and slices > 2 and own == 8 and own >= SWEEPS + slices - 2 \
        and rows == own * slices * count and cols % 128 == 0


def solution(mesh):
    slices, count = mesh.shape["tm"], mesh.shape["space"]
    plan = make_plan(slices)

    def wide(initial_state, capacity, source, control, segment_index):
        planes, rows, cols = initial_state.shape
        own = rows // (slices * count)
        total, window, parts = planes * count, 3 * own, cols // 128
        still = (total, parts, window + 16, 128)
        size = (planes, rows, cols, slices, count, own)
        dma = pltpu.SemaphoreType.DMA

        def fields(number):
            return pltpu.VMEM((number, total + 2, parts, window + 16, 128), jnp.float32)

        result = pl.pallas_call(
            functools.partial(wide_kernel, size),
            out_shape=jax.ShapeDtypeStruct((planes, rows // own, parts, own, 128), jnp.float32),
            in_specs=[pl.BlockSpec(memory_space=pl.ANY)] * 3 + [pl.BlockSpec(memory_space=pltpu.VMEM)] * 2,
            out_specs=pl.BlockSpec(memory_space=pl.ANY),
            scratch_shapes=[
                pltpu.VMEM((3, planes, parts, rows, 128), jnp.float32),
                fields(3),
                pltpu.VMEM(still, jnp.float32),
                pltpu.VMEM(still, jnp.float32),
                pltpu.VMEM((slices, total, parts, 8, 128), jnp.float32),
                fields(slices - 2),
                fields(4 * (slices - 1)),
                pltpu.VMEM((2 * (slices - 1),) + still, jnp.float32),
                fields(slices - 1),
                fields(2 * (slices - 2)),
                fields(slices - 1),
                fields(slices - 1),
                pltpu.VMEM((count,) + segment_index.shape, jnp.int32),
                pltpu.VMEM((slices,) + control.shape, jnp.float32),
                dma((3, parts)),
                dma((3, parts)),
                dma((3, count)),
                dma((3, count)),
                dma((count,)),
                dma((count,)),
                dma((slices,)),
                dma((slices,)),
                dma((3, 2)),
                dma((3, 2)),
                dma((slices - 1, 2)),
                dma((slices - 1, 2)),
                dma((slices, count)),
                dma((slices, count)),
                dma((3,)),
                pltpu.SemaphoreType.REGULAR((max(count // 2 - 2, 1),)),
                pltpu.SemaphoreType.REGULAR((slices // 2,)),
            ],
            compiler_params=pltpu.CompilerParams(
                collective_id=0, has_side_effects=True, vmem_limit_bytes=67043328 - 1048576
            ),
        )(initial_state, capacity, source, control, segment_index)
        return result.transpose(0, 1, 3, 2, 4).reshape(1, planes, rows, cols)

    def on_device(initial_state, capacity, source, control, segment_index):
        planes, rows, cols = initial_state.shape
        if wide_fits(slices, count, rows, cols):
            return wide(initial_state, capacity, source, control, segment_index)
        own_rows = rows // slices
        reach = -(-(CORRECTIONS * SWEEPS + slices - CORRECTIONS) // 8) * 8
        window = min(rows, own_rows + 2 * reach)
        fields = len(plan[0])
        size = (planes, window, own_rows, reach, rows, cols, slices, count)
        block = (planes, window, cols)
        dma = pltpu.SemaphoreType.DMA
        return pl.pallas_call(
            functools.partial(kernel, plan, size),
            out_shape=jax.ShapeDtypeStruct((1, planes, rows, cols), jnp.float32),
            in_specs=[pl.BlockSpec(memory_space=pl.ANY)] * 3 + [pl.BlockSpec(memory_space=pltpu.VMEM)] * 2,
            out_specs=pl.BlockSpec(memory_space=pl.ANY),
            scratch_shapes=[
                pltpu.VMEM((fields, planes + 2, window, cols), jnp.float32),
                pltpu.VMEM((slices,) + block, jnp.float32),
                pltpu.VMEM((2 * slices,) + block, jnp.float32),
                pltpu.VMEM(block, jnp.float32),
                pltpu.VMEM(block, jnp.float32),
                pltpu.VMEM(block, jnp.float32),
                pltpu.VMEM((slices,) + control.shape, jnp.float32),
                dma((fields, 2)),
                dma((fields, 2)),
                dma((3,)),
                dma((slices,)),
                dma((slices,)),
                dma((slices,)),
                dma((slices,)),
                dma((2,)),
            ],
            compiler_params=pltpu.CompilerParams(
                collective_id=0, has_side_effects=True, vmem_limit_bytes=67043328 - 1048576
            ),
        )(initial_state, capacity, source, control, segment_index)

    return jax.shard_map(
        on_device,
        mesh=mesh,
        in_specs=(
            P("space", None, None),
            P("space", None, None),
            P("space", None, None),
            P("tm", None),
            P("space", None),
        ),
        out_specs=P("tm", "space", None, None),
        check_vma=False,
    )
```
